512 devices in a mesh: section: 4 (over x), ctx: 16 (over z, y_hi), dp: 8 (over y_lo, core).
Axes of the slice: x: 4, y: 8 (y_hi: 2, y_lo: 4; y = y_hi * 4 + y_lo), z: 8, core: 2. Of those that a mesh axis runs over, the one named last changes fastest.
Arguments:
- first_input: bfloat16 [4, 8, 2048, 2048], P('section', 'dp', 'ctx'), may hold values from -14 to 14
- second_input: bfloat16 [4, 8, 2048, 2048], P('section', 'dp', 'ctx'), may hold values from -6 to 6
- upstream: bfloat16 [4, 8, 2048, 2048], P('section', 'dp', 'ctx'), may hold values from -6 to 6
- first_picks: int32 [4, 8, 2048, 6], P('section', 'dp', 'ctx'), may hold values from 0 to 63, all different within a row
- second_picks: int32 [4, 8, 2048, 6], P('section', 'dp', 'ctx'), may hold values from 0 to 63, all different within a row
- gate_grads: float32 [4, 8, 2048, 6], P('section', 'dp', 'ctx'), may hold values from -0.0009 to 0.0009
- norm_gain: float32 [4, 2048], P('section'), may hold values from 0.5 to 1.5
- router_weight: float32 [4, 64, 2048], P('section'), may hold values from -0.25 to 0.25
- gate_weight: bfloat16 [4, 2048, 1280], P('section', 'ctx'), may hold values from -0.125 to 0.125
- up_weight: bfloat16 [4, 2048, 1280], P('section', 'ctx'), may hold values from -0.125 to 0.125
- down_weight: bfloat16 [4, 1280, 2048], P('section', None, 'ctx'), may hold values from -0.15625 to 0.15625
Outputs:
- arrived: bfloat16 [4, 8, 2048, 2048], P('section', 'dp', 'ctx')
- routing: float32 [4, 8, 2048, 6], P('section', 'dp', 'ctx')
- input_grad: bfloat16 [4, 8, 2048, 2048], P('section', 'dp', 'ctx')
- router_grad: float32 [4, 64, 2048], P('section')
- balance: float32 [4, 8, 2], P('section', 'dp')
The draws below stay inside these ranges and needn't reach their ends.
Inputs may be any that keep to these rules, and one draw needn't show every extreme that they name: `first_picks`: each token names 6 different experts. `second_picks`: each token names 6 different experts.
All inputs are finite; a program needn't handle non-finite values.
Results may differ from the reference program's by a relative error of at most 0.002.
The reference program's roundings to bfloat16 on the way (of `normed` and `hidden`) count: a program that leaves them out, or rounds other values in their place, can miss the bound.
Values may be sent and summed in bfloat16 or wider, within the bound.
A program may use at most 64 MiB of HBM per device.

```python
import jax
import jax.numpy as jnp
from jax import lax

D = 2048
F = 1280
E = 64
TOP = 6
SEQ = 2048
SEQS = 8
SECTIONS = 4


def draw_first_input(key, part):
    common = jax.random.normal(jax.random.fold_in(key, 7), (SECTIONS, 1, 1, D), jnp.float32)
    noise = jax.random.normal(jax.random.fold_in(key, 13), (SECTIONS, SEQS, SEQ, D), jnp.float32)
    values = noise + 1.5 * common
    return jnp.clip(values, -14.0, 14.0).astype(jnp.bfloat16)


def levels(stream_key, shape, cuts, smallest, high):
    loudness, own = 1.0, jax.random.fold_in(stream_key, 6)
    for axis_at, blocks in cuts:
        draws = jnp.exp(jax.random.uniform(jax.random.fold_in(own, axis_at), (blocks,), jnp.float32, smallest / len(cuts), high / len(cuts)))
        loudness = loudness * jnp.repeat(draws, shape[axis_at] // blocks).reshape([-1 if axis == axis_at else 1 for axis in range(len(shape))])
    return loudness


def distinct(own_key, rows, amount, top, lift):
    sequence = jax.random.permutation(jax.random.fold_in(own_key, 1), amount)
    favour = sequence
    for power in range(3):
        favour = favour * favour // amount
    favour = favour * lift // amount
    chance = jax.random.randint(jax.random.fold_in(own_key, 2), (rows, amount), 0, 4096) + favour
    sure = jax.random.permutation(jax.random.fold_in(own_key, 3), rows)[jnp.arange(amount) % rows]
    chance = jnp.where(jnp.arange(rows)[:, None] == sure[None, :], 1 << 14, chance)
    priority = chance * amount + jnp.arange(amount)
    return lax.top_k(priority.astype(jnp.int32), top)[1].astype(jnp.int32)


def bell_draw(rng, extent, width, limit, cuts=(), kind=jnp.bfloat16):
    values = jax.random.normal(rng, extent, jnp.float32) * width
    if len(cuts) > 0:
        values = levels(rng, extent, cuts, -0.22, 0.18) * values
    return jnp.clip(values, min=-limit, max=limit).astype(kind)


def setup_inputs(seed: int = 0) -> dict:
    keys = jax.random.split(jax.random.key(seed), 12)
    first_input = draw_first_input(jax.random.fold_in(keys[11], 71), 0)
    second_input = bell_draw(keys[1], (SECTIONS, SEQS, SEQ, D), 1.0, 6.0, ((0, 4), (1, 8), (2, 16)))
    upstream = bell_draw(keys[2], (SECTIONS, SEQS, SEQ, D), 1.0, 6.0, ((0, 4), (1, 8), (2, 16)))
    first_picks = distinct(keys[3], SECTIONS * SEQS * SEQ, E, TOP, 768).reshape((SECTIONS, SEQS, SEQ, TOP))
    second_picks = distinct(keys[4], SECTIONS * SEQS * SEQ, E, TOP, 768).reshape((SECTIONS, SEQS, SEQ, TOP))
    gate_grads = bell_draw(keys[5], (SECTIONS, SEQS, SEQ, TOP), 0.00015, 0.0009, ((0, 4), (1, 8), (2, 16)), jnp.float32)
    norm_gain = jnp.clip(1.0 + 0.1 * jax.random.normal(keys[6], (SECTIONS, D), jnp.float32), 0.5, 1.5)
    router_weight = bell_draw(keys[7], (SECTIONS, E, D), (D // 4) ** -0.5, 0.25, ((0, 4),), jnp.float32)
    gate_weight = bell_draw(keys[8], (SECTIONS, D, F), D ** -0.5, 0.125, ((0, 4), (1, 16)))
    up_weight = bell_draw(keys[9], (SECTIONS, D, F), D ** -0.5, 0.125, ((0, 4), (1, 16)))
    down_weight = bell_draw(keys[10], (SECTIONS, F, D), F ** -0.5, 0.15625, ((0, 4), (2, 16)))
    return {"first_input": first_input, "second_input": second_input, "upstream": upstream, "first_picks": first_picks, "second_picks": second_picks, "gate_grads": gate_grads, "norm_gain": norm_gain, "router_weight": router_weight, "gate_weight": gate_weight, "up_weight": up_weight, "down_weight": down_weight}


EPSILON = 1e-06
ROUTE_SCALE = 2.5

def normalize(values_in, norm_gain):
    values = values_in.astype(jnp.float32)
    inverse = lax.rsqrt(lax.optimization_barrier(jnp.mean(values * values, axis=-1, keepdims=True)) + EPSILON)
    return ((values * inverse * norm_gain).astype(jnp.bfloat16), inverse)

def one_hot(picks, experts):
    labels = jnp.arange(experts, dtype=jnp.int32)
    return (picks[:, :, None] == labels[None, None, :]).astype(jnp.float32)

def scores(normed, router_w, table):
    logits = jnp.dot(normed.astype(jnp.float32), router_w.T, precision=lax.Precision.HIGHEST)
    affinity = jax.nn.sigmoid(logits)
    chosen = jnp.einsum('tke,te->tk', table, affinity, precision=lax.Precision.HIGHEST)
    chosen_sum = lax.optimization_barrier(jnp.sum(chosen, axis=-1, keepdims=True))
    gate_weights = ROUTE_SCALE * chosen / chosen_sum
    spread = lax.optimization_barrier(jnp.sum(affinity, axis=-1, keepdims=True))
    shares = affinity / spread
    return (affinity, chosen, chosen_sum, gate_weights, spread, shares)

def router_back(grads, table, affinity, chosen, chosen_sum, spread, shares, frac, length):
    chosen_grad = ROUTE_SCALE * (grads / chosen_sum - lax.optimization_barrier(jnp.sum(grads * chosen, axis=-1, keepdims=True)) / (chosen_sum * chosen_sum))
    affinity_grad = jnp.einsum('tk,tke->te', chosen_grad, table, precision=lax.Precision.HIGHEST)
    share_grad = frac[None, :] / length
    affinity_grad = affinity_grad + (share_grad - lax.optimization_barrier(jnp.sum(share_grad * shares, axis=-1, keepdims=True))) / spread
    return affinity_grad * affinity * (1.0 - affinity)

def shared_back(hidden_grad, gate_pre, up_pre):
    sigmoid_v = jax.nn.sigmoid(gate_pre)
    slope = sigmoid_v * (1.0 + gate_pre * (1.0 - sigmoid_v))
    gate_grad = (hidden_grad * up_pre * slope).astype(jnp.bfloat16)
    up_grad = (hidden_grad * gate_pre * sigmoid_v).astype(jnp.bfloat16)
    return (gate_grad, up_grad)

def norm_back(values_in, inverse, norm_gain, normed_grad):
    values = values_in.astype(jnp.float32)
    scaled = normed_grad * norm_gain
    return inverse * (scaled - values * inverse * inverse * lax.optimization_barrier(jnp.mean(scaled * values, axis=-1, keepdims=True)))

def window(first_in, second_in, returned, first_pk, second_pk, grads, norm_gain, router_w, gate_w, up_w, down_w):
    length = first_in.shape[0]
    experts = router_w.shape[0]
    per_token = first_pk.shape[1]
    normed_a, inverse_a = normalize(first_in, norm_gain)
    normed_b, inverse_b = normalize(second_in, norm_gain)
    table_a = one_hot(first_pk, experts)
    table_b = one_hot(second_pk, experts)
    aff_a, chosen_a, csum_a, routing_a, spread_a, shares_a = scores(normed_a, router_w, table_a)
    aff_b, chosen_b, csum_b, routing_b, spread_b, shares_b = scores(normed_b, router_w, table_b)
    frac_a = experts / (per_token * length) * lax.optimization_barrier(jnp.sum(table_a, axis=(0, 1)))
    frac_b = experts / (per_token * length) * lax.optimization_barrier(jnp.sum(table_b, axis=(0, 1)))
    balance = jnp.stack([jnp.sum(frac_a * lax.optimization_barrier(jnp.sum(shares_a, axis=0)) / length), jnp.sum(frac_b * lax.optimization_barrier(jnp.sum(shares_b, axis=0)) / length)])
    stacked = jnp.concatenate([normed_a, normed_b], axis=0)
    gate_pre = jnp.dot(stacked, gate_w, preferred_element_type=jnp.float32)
    up_pre = jnp.dot(stacked, up_w, preferred_element_type=jnp.float32)
    hidden = (jax.nn.silu(gate_pre) * up_pre).astype(jnp.bfloat16)
    output_a = (first_in.astype(jnp.float32) + jnp.dot(hidden[:length], down_w, preferred_element_type=jnp.float32)).astype(jnp.bfloat16)
    hidden_grad = jnp.dot(returned, down_w.T, preferred_element_type=jnp.float32)
    gate_grad, up_grad = shared_back(hidden_grad, gate_pre[length:], up_pre[length:])
    normed_grad = jnp.dot(gate_grad, gate_w.T, preferred_element_type=jnp.float32) + jnp.dot(up_grad, up_w.T, preferred_element_type=jnp.float32)
    logit_grad = router_back(grads, table_b, aff_b, chosen_b, csum_b, spread_b, shares_b, frac_b, length)
    router_part = jnp.dot(logit_grad.T, normed_b.astype(jnp.float32), precision=lax.Precision.HIGHEST)
    normed_grad = normed_grad + jnp.dot(logit_grad, router_w, precision=lax.Precision.HIGHEST)
    input_grad = (returned.astype(jnp.float32) + norm_back(second_in, inverse_b, norm_gain, normed_grad)).astype(jnp.bfloat16)
    return (output_a, routing_a, input_grad, router_part, balance)

def reference(first_input, second_input, upstream, first_picks, second_picks, gate_grads, norm_gain, router_weight, gate_weight, up_weight, down_weight):
    returned_all = jnp.roll(upstream, -1, axis=0)

    def per_section(section_args):
        first_in, second_in, returned, first_pk, second_pk, grads, gain_s, router_s, gate_s, up_s, down_s = section_args

        def per_seq(seq_args):
            return window(*seq_args, gain_s, router_s, gate_s, up_s, down_s)
        return lax.map(per_seq, (first_in, second_in, returned, first_pk, second_pk, grads))
    outputs, routing, input_grad, router_parts, balance = lax.map(per_section, (first_input, second_input, returned_all, first_picks, second_picks, gate_grads, norm_gain, router_weight, gate_weight, up_weight, down_weight))
    arrived = jnp.roll(outputs, 1, axis=0)
    return (arrived, routing, input_grad, lax.optimization_barrier(jnp.sum(router_parts, axis=1)), balance)
```

```python
import jax
import jax.numpy as jnp
from jax import lax
from jax.experimental import pallas as pl
from jax.experimental.pallas import tpu as pltpu
from jax.sharding import Mesh
from jax.sharding import PartitionSpec as P

CTX = ("ctx_0", "ctx_1")
MESH = pl.DeviceIdType.MESH
EPSILON = 1e-06
ROUTE_SCALE = 2.5
HIGH = lax.Precision.HIGHEST
F32 = jnp.float32
BF16 = jnp.bfloat16

NZ, NY, NX = 8, 8, 4
GZ, DZ = 14, 7
GY, DY = 16, 8
NZP, NYP = GZ + DZ, GY + DY
LA, LB = 1, 2

NT = (((1,), (1,)), ((), ()))
TN = (((0,), (0,)), ((), ()))
NN = (((1,), (0,)), ((), ()))


def dot(a, b, dims=NN, precision=None):
    return lax.dot_general(a, b, dims, precision=precision, preferred_element_type=F32)


def sigmoid(v):
    return jax.nn.sigmoid(v)


def kernel(
    first, second, upstream, picks_a, picks_b, grads, gain, router_w, gate, up, down,
    arrived, routing, input_grad, router_grad, balance,
    wgu, wd, returned, normed, inverse, gacc, uacc, hgrad, hid, gg, ug, out, qbuf,
    cnt_src, cnt, aff, csum, spread, logit,
    rp, r0, b0, b1, r1, b2, r2, r3,
    local_sem, zsend, zrecv, ysend, yrecv, dzsend, dzrecv, dysend, dyrecv,
    xsem, osend, orecv, csend, crecv, rsend, rrecv,
):
    d_model = gate.shape[0] * 2 * NZ
    hidden = gate.shape[1]
    tokens = first.shape[0]
    rows_s = gate.shape[0]
    pg, pd = rows_s // 4, hidden // 2
    block = 2 * rows_s
    length = tokens * 2 * NZ

    x = lax.axis_index("section")
    z = lax.axis_index("ctx_0")
    h = lax.axis_index("ctx_1")
    dp = lax.axis_index("dp")
    j = dp // 2
    c = dp % 2
    y = h * 4 + j
    sgn = 1 - 2 * c

    def dev(xx, zz, yy, cc):
        return (xx, zz, yy // 4, (yy % 4) * 2 + cc)

    partner = dev(x, z, y, 1 - c)
    z_next = dev(x, (z + sgn + NZ) % NZ, y, c)
    y_next = dev(x, z, (y + sgn + NY) % NY, c)
    x_next = dev((x + 1) % NX, z, y, c)
    x_prev = dev((x + NX - 1) % NX, z, y, c)

    def z_peer(r):
        return dev(x, (z + r) % NZ, y, c)

    def y_peer(r):
        return dev(x, z, (y + r) % NY, c)

    def c_peer(r):
        rank = (z * 2 + h + r) % (2 * NZ)
        return (x, rank // 2, rank % 2, dp)

    def remote(src, dst, send, recv, device):
        return pltpu.make_async_remote_copy(
            src_ref=src, dst_ref=dst, send_sem=send, recv_sem=recv, device_id=device, device_id_type=MESH
        )

    barrier = pltpu.get_barrier_semaphore()

    def greet(device):
        pl.semaphore_signal(barrier, inc=1, device_id=device, device_id_type=MESH)

    greet(partner)
    greet(x_next)
    greet(x_prev)
    for r in range(1, 2 * NZ):
        greet(c_peer(r))
    for r in range(1, NY):
        if r != 4:
            greet(y_peer(r))

    own = z * 2 + h
    own_rows = pl.ds(pl.multiple_of(own * rows_s, rows_s), rows_s)
    local = [
        pltpu.make_async_copy(gate, wgu.at[0, own_rows, :], local_sem.at[0]),
        pltpu.make_async_copy(up, wgu.at[1, own_rows, :], local_sem.at[1]),
        pltpu.make_async_copy(down, wd.at[:, own_rows], local_sem.at[2]),
    ]
    for copy in local:
        copy.start()
    for copy in local:
        copy.wait()
    pl.semaphore_wait(barrier, 3 + 2 * NZ - 1 + NY - 2)

    def g_piece(slot, p):
        start = pl.multiple_of(slot * rows_s + p * pg, pg)
        return wgu.at[:, pl.ds(start, pg), :]

    def d_piece(slot, p):
        return wd.at[pl.ds(pl.multiple_of(p * pd, pd), pd), pl.ds(pl.multiple_of(slot * rows_s, rows_s), rows_s)]

    def slot_of(zz, hh):
        return ((zz + 2 * NZ) % NZ) * 2 + hh

    def zg_ref(n, core, sign):
        return g_piece(slot_of(z - sign * (n // 4 + 1), h), (2 * core + n % 4) % 4)

    def zd_ref(n, core, sign):
        return d_piece(slot_of(z - sign * (n // 2 + 1), h), (core + n % 2) % 2)

    def y_offset(q, sign):
        return (1 - 2 * (q % 2)) * ((q + 1) // 2) * sign

    def yg_ref(n, core, sign, hh):
        return g_piece(slot_of(z + y_offset(n // 2, sign), hh), 2 * core + n % 2)

    def yd_ref(n, core, sign, hh):
        return d_piece(slot_of(z + y_offset(n, sign), hh), core)

    def zg_send(n):
        ref = g_piece(slot_of(z - sgn * (n // 4), h), (2 * c + n % 4) % 4)
        return remote(ref, ref, zsend.at[n], zrecv.at[n], z_next)

    def zd_send(n):
        ref = d_piece(slot_of(z - sgn * (n // 2), h), (c + n % 2) % 2)
        return remote(ref, ref, zsend.at[GZ + n], zrecv.at[GZ + n], z_next)

    last = 3 * (1 - c)
    is_last = j == last
    hops = jnp.where(c == 0, j + 1, 4 - j)
    hops_max = jnp.maximum(hops, 5 - hops)
    send_half = jnp.where(is_last, h, 1 - h)

    def yg_send(n):
        ref = yg_ref(n, c, sgn, send_half)
        return remote(ref, ref, ysend.at[n], yrecv.at[n], y_next)

    def yd_send(n):
        ref = yd_ref(n, c, sgn, send_half)
        return remote(ref, ref, ysend.at[GY + n], yrecv.at[GY + n], y_next)

    for n in range(4):
        zg_send(n).start()

    @pl.when(is_last)
    def _():
        for n in range(2):
            yg_send(n).start()

    back = remote(upstream, returned, xsem.at[0], xsem.at[1], x_prev)
    back.start()

    step_rows = 16

    def norm_rows(source, base):
        def body(i, _):
            rows = pl.ds(pl.multiple_of(i * step_rows, step_rows), step_rows)
            values = source[rows, :].astype(F32)
            inv = lax.rsqrt(jnp.mean(values * values, axis=-1, keepdims=True) + EPSILON)
            inverse[pl.ds(pl.multiple_of(base + i * step_rows, step_rows), step_rows), :] = jnp.broadcast_to(inv, (step_rows, 128))
            scaled = (values * inv * gain[...]).astype(BF16)
            for b in range(d_model // block):
                normed[b, pl.ds(pl.multiple_of(base + i * step_rows, step_rows), step_rows), :] = scaled[:, b * block : (b + 1) * block]
            return 0

        lax.fori_loop(0, tokens // step_rows, body, 0)

    norm_rows(first, 0)
    norm_rows(second, tokens)
    gacc[...] = jnp.zeros_like(gacc)
    uacc[...] = jnp.zeros_like(uacc)
    hgrad[...] = jnp.zeros_like(hgrad)

    experts = router_w.shape[0]
    top = picks_a.shape[0]
    logits = jnp.zeros((experts, 2 * tokens), F32)
    for b in range(d_model // block):
        logits = logits + dot(
            router_w[:, b * block : (b + 1) * block], normed[b].astype(F32), NT, HIGH
        )
    affinity = sigmoid(logits)
    aff[...] = affinity
    labels = lax.broadcasted_iota(jnp.int32, (experts, tokens), 0)

    def picked(picks, affinities, k):
        hit = picks[k : k + 1, :] == labels
        return jnp.sum(jnp.where(hit, affinities, 0.0), axis=0, keepdims=True), hit

    stats = []
    for m, picks in enumerate((picks_a, picks_b)):
        part = affinity[:, m * tokens : (m + 1) * tokens]
        tab = jnp.zeros((experts, tokens), F32)
        chosen = []
        for k in range(top):
            value, hit = picked(picks, part, k)
            chosen.append(value)
            tab = tab + jnp.where(hit, 1.0, 0.0)
        total = chosen[0]
        for value in chosen[1:]:
            total = total + value
        all_aff = jnp.sum(part, axis=0, keepdims=True)
        if m == 0:
            for k in range(top):
                routing[k : k + 1, :] = ROUTE_SCALE * chosen[k] / total
        else:
            csum[...] = total
            spread[...] = all_aff
        stats.append((tab, part / all_aff))
    ones = jnp.ones((8, tokens), F32)
    counts_row = dot(ones, jnp.concatenate([stats[0][0], stats[1][0]], axis=0), NT, HIGH)
    shares_row = dot(ones, jnp.concatenate([stats[0][1], stats[1][1]], axis=0), NT, HIGH)
    row_id = lax.broadcasted_iota(jnp.int32, (8, 2 * experts), 0)
    packed = jnp.where(row_id == 0, counts_row, jnp.where(row_id == 1, shares_row, 0.0))
    cnt_src[...] = packed
    for r in range(1, 2 * NZ):
        remote(cnt_src, cnt.at[r], csend.at[r], crecv.at[r], c_peer(r)).start()

    half_e = experts // 2
    own_half = pl.ds(pl.multiple_of(c * half_e, half_e), half_e)
    other_half = pl.ds(pl.multiple_of((1 - c) * half_e, half_e), half_e)

    def cols(i, width):
        return pl.ds(pl.multiple_of(i * width, width), width)

    def rs_pair():
        return remote(rp.at[other_half, :], b0, rsend.at[0], rrecv.at[0], partner)

    def rs_z(r):
        return remote(
            r0.at[:, cols((z + r) % NZ, block)], b1.at[r], rsend.at[r], rrecv.at[r], z_peer(r)
        )

    def tile(yy):
        return (cols(yy // 2, 8), cols(yy % 2, 128))

    def rs_y(r):
        return remote(r1.at[tile((y + r) % NY)], b2.at[r], rsend.at[8 + r], rrecv.at[8 + r], y_peer(r))

    def ag_y(r):
        return remote(r2, r3.at[tile(y)], rsend.at[16 + r], rrecv.at[16 + r], y_peer(r))

    def ag_z(r):
        return remote(
            r3, router_grad.at[own_half, cols(z, block)], rsend.at[24 + r], rrecv.at[24 + r], z_peer(r)
        )

    def ag_pair():
        return remote(
            router_grad.at[own_half, :], router_grad.at[own_half, :], rsend.at[32], rrecv.at[32], partner
        )

    def router_0():
        for r in range(1, 2 * NZ):
            remote(cnt_src, cnt.at[r], csend.at[r], crecv.at[r], c_peer(r)).wait_recv()
        totals = cnt_src[...]
        for r in range(1, 2 * NZ):
            totals = totals + cnt[r]
        scale = experts / (top * length)
        frac = scale * totals[0:1, :]
        terms = frac * totals[1:2, :] / length
        lane = lax.broadcasted_iota(jnp.int32, (1, 2 * experts), 1)
        bal_a = jnp.sum(jnp.where(lane < experts, terms, 0.0), axis=1, keepdims=True)
        bal_b = jnp.sum(jnp.where(lane >= experts, terms, 0.0), axis=1, keepdims=True)
        balance[...] = jnp.where(lane == 0, bal_a, bal_b)[:, 0:2]
        e_sub = lax.broadcasted_iota(jnp.int32, (experts, 2 * experts), 0)
        e_lane = lax.broadcasted_iota(jnp.int32, (experts, 2 * experts), 1)
        frac_col = jnp.sum(jnp.where(e_lane == e_sub + experts, frac, 0.0), axis=1, keepdims=True)
        aff_b = aff[:, tokens : 2 * tokens]
        chosen_sum = csum[...]
        shares = aff_b / spread[...]
        inner = jnp.zeros((1, tokens), F32)
        for k in range(top):
            value, _ = picked(picks_b, aff_b, k)
            inner = inner + grads[k : k + 1, :] * value
        agrad = jnp.zeros((experts, tokens), F32)
        for k in range(top):
            hit = picks_b[k : k + 1, :] == labels
            cgrad = ROUTE_SCALE * (grads[k : k + 1, :] / chosen_sum - inner / (chosen_sum * chosen_sum))
            agrad = agrad + jnp.where(hit, cgrad, 0.0)
        share_grad = frac_col / length
        agrad = agrad + (share_grad - jnp.sum(share_grad * shares, axis=0, keepdims=True)) / spread[...]
        lg = agrad * aff_b * (1.0 - aff_b)
        logit[...] = lg
        for b in range(d_model // block):
            rp[:, b * block : (b + 1) * block] = dot(
                lg, normed[b, tokens : 2 * tokens, :].astype(F32), NN, HIGH
            )
        rs_pair().start()

    def router_1():
        rs_pair().wait_recv()
        r0[...] = rp[own_half, :] + b0[...]
        for r in range(1, NZ):
            rs_z(r).start()

    def router_2():
        for r in range(1, NZ):
            rs_z(r).wait_recv()
        acc = r0[:, cols(z, block)]
        for r in range(1, NZ):
            acc = acc + b1[r]
        r1[...] = acc
        for r in range(1, NY):
            rs_y(r).start()

    def router_3():
        for r in range(1, NY):
            rs_y(r).wait_recv()
        acc = r1[tile(y)]
        for r in range(1, NY):
            acc = acc + b2[r]
        r2[...] = acc
        r3[tile(y)] = acc
        for r in range(1, NY):
            ag_y(r).start()

    def router_4():
        for r in range(1, NY):
            ag_y(r).wait_recv()
        router_grad[own_half, cols(z, block)] = r3[...]
        for r in range(1, NZ):
            ag_z(r).start()

    def router_5():
        for r in range(1, NZ):
            ag_z(r).wait_recv()
        ag_pair().start()

    router_at = {3: router_0, 5: router_1, 9: router_2, 11: router_3, 14: router_4, 19: router_5}

    n_tile = 256

    def z_rows(zz):
        return pl.ds(pl.multiple_of(zz * block, block), block)

    def g_block(zz):
        lhs = normed[zz]
        for n in range(hidden // n_tile):
            at = slice(n * n_tile, (n + 1) * n_tile)
            gacc[:, at] += dot(lhs, wgu[0, z_rows(zz), at])
            uacc[:, at] += dot(lhs, wgu[1, z_rows(zz), at])

    def make_hidden():
        def body(i, _):
            rows = cols(i, 16)
            v = gacc[rows, :]
            hid[rows, :] = (v * sigmoid(v) * uacc[rows, :]).astype(BF16)
            return 0

        lax.fori_loop(0, tokens // 16, body, 0)

    def out_send(zz):
        return remote(
            out.at[:, z_rows(zz)], arrived.at[:, z_rows(zz)], osend.at[zz], orecv.at[zz], x_next
        )

    def d_block(zz):
        acc = dot(hid[...], wd[:, z_rows(zz)])
        out[:, z_rows(zz)] = (first[:, z_rows(zz)].astype(F32) + acc).astype(BF16)
        out_send(zz).start()
        lhs = returned[:, z_rows(zz)]
        for n in range(hidden // n_tile):
            at = slice(n * n_tile, (n + 1) * n_tile)
            hgrad[:, at] += dot(lhs, wd[at, z_rows(zz)], NT)

    def consume(fn, group):
        @pl.when(group == 0)
        def _():
            fn(z)

        @pl.when((group > 0) & (group < 4))
        def _():
            fn((z + group) % NZ)
            fn((z - group + NZ) % NZ)

        @pl.when(group == 4)
        def _():
            fn((z + 4) % NZ)

    def slot(t, _):
        nz = t - 1

        @pl.when((nz >= 0) & (nz < GZ))
        def _():
            ref = zg_ref(nz, c, sgn)
            remote(ref, ref, zsend.at[nz], zrecv.at[nz], z_next).wait_recv()
            remote(ref, ref, dzsend.at[nz], dzrecv.at[nz], partner).start()

            @pl.when(nz < GZ - 4)
            def _():
                zg_send(nz + 4).start()

            @pl.when(nz == GZ - 4)
            def _():
                zd_send(0).start()

            @pl.when(nz == GZ - 3)
            def _():
                zd_send(1).start()

        @pl.when((nz >= GZ) & (nz < NZP))
        def _():
            n = nz - GZ
            ref = zd_ref(n, c, sgn)
            remote(ref, ref, zsend.at[nz], zrecv.at[nz], z_next).wait_recv()
            remote(ref, ref, dzsend.at[nz], dzrecv.at[nz], partner).start()

            @pl.when(n < DZ - 2)
            def _():
                zd_send(n + 2).start()

        ndz = t - 3

        @pl.when((ndz >= 0) & (ndz < GZ))
        def _():
            ref = zg_ref(ndz, 1 - c, -sgn)
            remote(ref, ref, dzsend.at[ndz], dzrecv.at[ndz], partner).wait_recv()

        @pl.when((ndz >= GZ) & (ndz < NZP))
        def _():
            ref = zd_ref(ndz - GZ, 1 - c, -sgn)
            remote(ref, ref, dzsend.at[ndz], dzrecv.at[ndz], partner).wait_recv()

        nyr = t - LA - LB * hops

        @pl.when((nyr >= 0) & (nyr < GY))
        def _():
            ref = yg_ref(nyr, c, sgn, 1 - h)
            remote(ref, ref, ysend.at[nyr], yrecv.at[nyr], y_next).wait_recv()
            remote(ref, ref, dysend.at[nyr], dyrecv.at[nyr], partner).start()

        @pl.when((nyr >= GY) & (nyr < NYP))
        def _():
            ref = yd_ref(nyr - GY, c, sgn, 1 - h)
            remote(ref, ref, ysend.at[nyr], yrecv.at[nyr], y_next).wait_recv()
            remote(ref, ref, dysend.at[nyr], dyrecv.at[nyr], partner).start()

        nys = jnp.where(is_last, t - 1, nyr)
        low = jnp.where(is_last, 2, 0)

        @pl.when((nys >= low) & (nys < GY))
        def _():
            yg_send(nys).start()

        @pl.when((nys >= GY) & (nys < NYP))
        def _():
            yd_send(nys - GY).start()

        nyd = t - LA - LB * hops_max - 1

        @pl.when((nyd >= 0) & (nyd < GY))
        def _():
            ref = yg_ref(nyd, 1 - c, -sgn, 1 - h)
            remote(ref, ref, dysend.at[nyd], dyrecv.at[nyd], partner).wait_recv()

            @pl.when((nyd % 4 == 1) | (nyd == GY - 1))
            def _():
                consume(g_block, (nyd + 1) // 4)

            @pl.when(nyd == GY - 1)
            def _():
                make_hidden()

        @pl.when((nyd >= GY) & (nyd < NYP))
        def _():
            n = nyd - GY
            ref = yd_ref(n, 1 - c, -sgn, 1 - h)
            remote(ref, ref, dysend.at[nyd], dyrecv.at[nyd], partner).wait_recv()

            @pl.when(n == 0)
            def _():
                back.wait_recv()

            @pl.when((n % 2 == 0) | (n == DY - 1))
            def _():
                consume(d_block, (n + 1) // 2)

        for at, stage in router_at.items():

            @pl.when(t == at)
            def _():
                stage()

        return 0

    lax.fori_loop(0, NYP + LA + LB * 4 + 1, slot, 0)

    def shared_back(i, _):
        rows = cols(i, 16)
        b_rows = pl.ds(pl.multiple_of(tokens + i * 16, 16), 16)
        v, u, hg = gacc[b_rows, :], uacc[b_rows, :], hgrad[rows, :]
        s = sigmoid(v)
        gg[rows, :] = (hg * u * (s * (1.0 + v * (1.0 - s)))).astype(BF16)
        ug[rows, :] = (hg * v * s).astype(BF16)
        return 0

    lax.fori_loop(0, tokens // 16, shared_back, 0)
    lg_t = jnp.transpose(logit[...])

    def grad_block(b, mean):
        at = z_rows(b)
        grad = dot(gg[...], wgu[0, at, :], NT) + dot(ug[...], wgu[1, at, :], NT)
        grad = grad + dot(lg_t, router_w[:, at], NN, HIGH)
        q = grad * gain[:, at]
        qbuf[b] = q
        return mean + jnp.sum(q * second[:, at].astype(F32), axis=-1, keepdims=True)

    mean = lax.fori_loop(0, d_model // block, grad_block, jnp.zeros((tokens, 1), F32)) / d_model
    inv_b = inverse[tokens : 2 * tokens, 0:1]
    factor = inv_b * inv_b * mean

    def final_block(b, _):
        at = z_rows(b)
        values = second[:, at].astype(F32)
        part = inv_b * (qbuf[b] - values * factor)
        input_grad[:, at] = (returned[:, at].astype(F32) + part).astype(BF16)
        return 0

    lax.fori_loop(0, d_model // block, final_block, 0)

    ag_pair().wait_recv()

    def drain(count, body):
        def step(n, _):
            body(n)
            return 0

        lax.fori_loop(0, count, step, 0)

    drain(2 * NZ // 2, lambda n: out_send(n).wait())
    drain(GZ, lambda n: zg_send(n).wait_send())
    drain(DZ, lambda n: zd_send(n).wait_send())
    drain(GY, lambda n: yg_send(n).wait_send())
    drain(DY, lambda n: yd_send(n).wait_send())

    def pair_done(ref, send, recv):
        remote(ref, ref, send, recv, partner).wait_send()

    drain(GZ, lambda n: pair_done(zg_ref(n, c, sgn), dzsend.at[n], dzrecv.at[n]))
    drain(DZ, lambda n: pair_done(zd_ref(n, c, sgn), dzsend.at[GZ + n], dzrecv.at[GZ + n]))
    drain(GY, lambda n: pair_done(yg_ref(n, c, sgn, 1 - h), dysend.at[n], dyrecv.at[n]))
    drain(DY, lambda n: pair_done(yd_ref(n, c, sgn, 1 - h), dysend.at[GY + n], dyrecv.at[GY + n]))
    back.wait_send()
    for r in range(1, 2 * NZ):
        remote(cnt_src, cnt.at[r], csend.at[r], crecv.at[r], c_peer(r)).wait_send()
    rs_pair().wait_send()
    ag_pair().wait_send()
    for r in range(1, NZ):
        rs_z(r).wait_send()
        ag_z(r).wait_send()
    for r in range(1, NY):
        rs_y(r).wait_send()
        ag_y(r).wait_send()


def shards(
    first_input, second_input, upstream, first_picks, second_picks, gate_grads,
    norm_gain, router_weight, gate_weight, up_weight, down_weight,
):
    tokens, d_model = first_input.shape[2:]
    hidden = gate_weight.shape[2]
    experts = router_weight.shape[1]
    top = first_picks.shape[3]
    block = d_model // NZ
    blocks = d_model // block
    vmem = pl.BlockSpec(memory_space=pltpu.VMEM)
    hbm = pl.BlockSpec(memory_space=pl.ANY)
    sem = pltpu.SemaphoreType.DMA
    half = experts // 2
    outs = pl.pallas_call(
        kernel,
        out_shape=(
            jax.ShapeDtypeStruct((tokens, d_model), BF16),
            jax.ShapeDtypeStruct((top, tokens), F32),
            jax.ShapeDtypeStruct((tokens, d_model), BF16),
            jax.ShapeDtypeStruct((experts, d_model), F32),
            jax.ShapeDtypeStruct((1, 2), F32),
        ),
        in_specs=[vmem, vmem, vmem, vmem, vmem, vmem, vmem, vmem, hbm, hbm, hbm],
        out_specs=(vmem,) * 5,
        scratch_shapes=[
            pltpu.VMEM((2, d_model, hidden), BF16),
            pltpu.VMEM((hidden, d_model), BF16),
            pltpu.VMEM((tokens, d_model), BF16),
            pltpu.VMEM((blocks, 2 * tokens, block), BF16),
            pltpu.VMEM((2 * tokens, 128), F32),
            pltpu.VMEM((2 * tokens, hidden), F32),
            pltpu.VMEM((2 * tokens, hidden), F32),
            pltpu.VMEM((tokens, hidden), F32),
            pltpu.VMEM((tokens, hidden), BF16),
            pltpu.VMEM((tokens, hidden), BF16),
            pltpu.VMEM((tokens, hidden), BF16),
            pltpu.VMEM((tokens, d_model), BF16),
            pltpu.VMEM((blocks, tokens, block), F32),
            pltpu.VMEM((8, 2 * experts), F32),
            pltpu.VMEM((2 * NZ, 8, 2 * experts), F32),
            pltpu.VMEM((experts, 2 * tokens), F32),
            pltpu.VMEM((1, tokens), F32),
            pltpu.VMEM((1, tokens), F32),
            pltpu.VMEM((experts, tokens), F32),
            pltpu.VMEM((experts, d_model), F32),
            pltpu.VMEM((half, d_model), F32),
            pltpu.VMEM((half, d_model), F32),
            pltpu.VMEM((NZ, half, block), F32),
            pltpu.VMEM((half, block), F32),
            pltpu.VMEM((NY, 8, 128), F32),
            pltpu.VMEM((8, 128), F32),
            pltpu.VMEM((half, block), F32),
            sem((3,)),
            sem((NZP,)), sem((NZP,)), sem((NYP,)), sem((NYP,)),
            sem((NZP,)), sem((NZP,)), sem((NYP,)), sem((NYP,)),
            sem((2,)), sem((NZ,)), sem((NZ,)),
            sem((2 * NZ,)), sem((2 * NZ,)), sem((33,)), sem((33,)),
        ],
        compiler_params=pltpu.CompilerParams(
            collective_id=0, has_side_effects=True, vmem_limit_bytes=60 * 1024 * 1024
        ),
    )(
        first_input[0, 0],
        second_input[0, 0],
        upstream[0, 0],
        first_picks[0, 0].T,
        second_picks[0, 0].T,
        gate_grads[0, 0].T,
        norm_gain,
        router_weight[0],
        gate_weight[0],
        up_weight[0],
        down_weight[0],
    )
    arrived, routing, input_grad, router_grad, balance = outs
    return (
        arrived[None, None],
        routing.T[None, None],
        input_grad[None, None],
        router_grad[None],
        balance[None],
    )


def solution(mesh):
    split = Mesh(
        mesh.devices.reshape(mesh.shape["section"], NZ, 2, mesh.shape["dp"]),
        ("section", "ctx_0", "ctx_1", "dp"),
    )
    tokens = P("section", "dp", CTX, None)
    return jax.shard_map(
        shards,
        mesh=split,
        in_specs=(tokens,) * 6
        + (
            P("section", None),
            P("section", None, None),
            P("section", CTX, None),
            P("section", CTX, None),
            P("section", None, CTX),
        ),
        out_specs=(tokens,) * 3 + (P("section", None, None), P("section", "dp", None)),
        check_vma=False,
    )
```

```python
import jax
import jax.numpy as jnp
from jax import lax
from jax.experimental import pallas as pl
from jax.experimental.pallas import tpu as pltpu
from jax.sharding import Mesh
from jax.sharding import PartitionSpec as P

CTX = ("ctx_0", "ctx_1")
MESH = pl.DeviceIdType.MESH
EPSILON = 1e-06
ROUTE_SCALE = 2.5
HIGH = lax.Precision.HIGHEST
F32 = jnp.float32
BF16 = jnp.bfloat16

NZ, NY, NX = 8, 8, 4
G, D = 0, 1
Z_ORDER = (
    [(G, 1, m) for m in range(4)]
    + [(G, 2, m) for m in range(4)]
    + [(D, 1, m) for m in range(2)]
    + [(G, 3, m) for m in range(4)]
    + [(D, 2, m) for m in range(2)]
    + [(G, 4, m) for m in range(2)]
    + [(D, 3, m) for m in range(2)]
    + [(D, 4, 0)]
)
Y_ORDER = [(G, 0, 0), (G, 0, 1), (D, 0, 0)]
for _q in ((G, 1), (G, 2), (G, 3), (G, 4), (D, 1), (D, 2), (G, 5), (G, 6), (D, 3), (D, 4), (G, 7), (D, 5), (D, 6), (D, 7)):
    Y_ORDER += [(_q[0], _q[1], m) for m in range(2 - _q[0])]
NZP, NYP = len(Z_ORDER), len(Y_ORDER)
Y_START = 3
LA, LB = 1, 2


def lookup(values, i):
    out = jnp.int32(values[0])
    for p in range(1, len(values)):
        if values[p] != values[p - 1]:
            out = jnp.where(i >= p, jnp.int32(values[p]), out)
    return out


def code(kind, k, m):
    return kind * 64 + k * 4 + m


def z_next_place(entry):
    kind, k, m = entry
    return Z_ORDER.index((kind, k + 1, m)) if (kind, k + 1, m) in Z_ORDER else -1

NT = (((1,), (1,)), ((), ()))
TN = (((0,), (0,)), ((), ()))
NN = (((1,), (0,)), ((), ()))


def dot(a, b, dims=NN, precision=None):
    return lax.dot_general(a, b, dims, precision=precision, preferred_element_type=F32)


def exact_dot(a, b, dims):
    rows = a.shape[0]
    one = a.astype(BF16)
    left = a - one.astype(F32)
    two = left.astype(BF16)
    three = (left - two.astype(F32)).astype(BF16)
    parts = dot(jnp.concatenate([one, two, three], axis=0), b, dims)
    return parts[2 * rows :] + parts[rows : 2 * rows] + parts[:rows]


def sigmoid(v):
    return jax.nn.sigmoid(v)


def kernel(
    first_hbm, second_hbm, upstream, picks_a, picks_b, grads, gain, router_hbm, gate, up, down,
    arrived, routing, input_grad, router_grad, balance,
    first, second, router_w, grad_out, routing_out, balance_out, wgu, wd, returned, normed, inverse, gacc, uacc, hgrad, hid, gg, ug, out, qbuf,
    cnt_src, cnt, aff, csum, spread, logit,
    rp, r0, b0, b1, r1, b2, r2, r3,
    local_sem, zsend, zrecv, ysend, yrecv, dzsend, dzrecv, dysend, dyrecv,
    xsem, osend, orecv, csend, crecv, rsend, rrecv,
):
    d_model = gate.shape[0] * 2 * NZ
    hidden = gate.shape[1]
    tokens = first_hbm.shape[0]
    rows_s = gate.shape[0]
    pg, pd = rows_s // 4, hidden // 2
    block = 2 * rows_s
    length = tokens * 2 * NZ

    x = lax.axis_index("section")
    z = lax.axis_index("ctx_0")
    h = lax.axis_index("ctx_1")
    dp = lax.axis_index("dp")
    j = dp // 2
    c = dp % 2
    y = h * 4 + j
    sgn = 1 - 2 * c

    def dev(xx, zz, yy, cc):
        return (xx, zz, yy // 4, (yy % 4) * 2 + cc)

    partner = dev(x, z, y, 1 - c)
    z_next = dev(x, (z + sgn + NZ) % NZ, y, c)
    z_prev = dev(x, (z - sgn + NZ) % NZ, y, c)
    y_next = dev(x, z, (y + sgn + NY) % NY, c)
    x_next = dev((x + 1) % NX, z, y, c)
    x_prev = dev((x + NX - 1) % NX, z, y, c)

    def z_peer(r):
        return dev(x, (z + r) % NZ, y, c)

    def y_peer(r):
        return dev(x, z, (y + r) % NY, c)

    def c_peer(r):
        rank = (z * 2 + h + r) % (2 * NZ)
        return (x, rank // 2, rank % 2, dp)

    def remote(src, dst, send, recv, device):
        return pltpu.make_async_remote_copy(
            src_ref=src, dst_ref=dst, send_sem=send, recv_sem=recv, device_id=device, device_id_type=MESH
        )

    barrier = pltpu.get_barrier_semaphore()

    def greet(device):
        pl.semaphore_signal(barrier, inc=1, device_id=device, device_id_type=MESH)

    greet(partner)
    greet(x_next)
    greet(x_prev)
    for r in range(1, 2 * NZ):
        greet(c_peer(r))
    for r in range(1, NY):
        if r != 4:
            greet(y_peer(r))

    own = z * 2 + h
    own_rows = pl.ds(pl.multiple_of(own * rows_s, rows_s), rows_s)
    local = [
        pltpu.make_async_copy(first_hbm, first, local_sem.at[0]),
        pltpu.make_async_copy(second_hbm, second, local_sem.at[1]),
        pltpu.make_async_copy(router_hbm, router_w, local_sem.at[2]),
        pltpu.make_async_copy(gate, wgu.at[0, own_rows, :], local_sem.at[3]),
        pltpu.make_async_copy(up, wgu.at[1, own_rows, :], local_sem.at[4]),
        pltpu.make_async_copy(down, wd.at[:, own_rows], local_sem.at[5]),
    ]
    for copy in local:
        copy.start()

    def g_piece(slot, p):
        start = pl.multiple_of(slot * rows_s + p * pg, pg)
        return wgu.at[:, pl.ds(start, pg), :]

    def d_piece(slot, p):
        return wd.at[pl.ds(pl.multiple_of(p * pd, pd), pd), pl.ds(pl.multiple_of(slot * rows_s, rows_s), rows_s)]

    def slot_of(zz, hh):
        return ((zz + 2 * NZ) % NZ) * 2 + hh

    def z_ref(kind, k, m, core, sign):
        slot = slot_of(z - sign * k, h)
        if kind == G:
            return g_piece(slot, (2 * core + m) % 4)
        return d_piece(slot, (core + m) % 2)

    def y_ref(kind, q, m, core, sign, hh):
        slot = slot_of(z + (1 - 2 * (q % 2)) * ((q + 1) // 2) * sign, hh)
        if kind == G:
            return g_piece(slot, 2 * core + m)
        return d_piece(slot, core)

    def z_copy(ref, place):
        return remote(ref, ref, zsend.at[place], zrecv.at[place], z_next)

    def y_copy(ref, place):
        return remote(ref, ref, ysend.at[place], yrecv.at[place], y_next)

    def dz_copy(ref, place):
        return remote(ref, ref, dzsend.at[place], dzrecv.at[place], partner)

    def dy_copy(ref, place):
        return remote(ref, ref, dysend.at[place], dyrecv.at[place], partner)

    last = 3 * (1 - c)
    is_last = j == last
    hops = jnp.where(c == 0, j + 1, 4 - j)
    hops_max = jnp.maximum(hops, 5 - hops)
    send_half = jnp.where(is_last, h, 1 - h)

    step_rows = 16

    def norm_rows(source, base):
        def body(i, _):
            rows = pl.ds(pl.multiple_of(i * step_rows, step_rows), step_rows)
            values = source[rows, :].astype(F32)
            inv = lax.rsqrt(jnp.mean(values * values, axis=-1, keepdims=True) + EPSILON)
            inverse[pl.ds(pl.multiple_of(base + i * step_rows, step_rows), step_rows), :] = jnp.broadcast_to(inv, (step_rows, 128))
            scaled = (values * inv * gain[...]).astype(BF16)
            for b in range(d_model // block):
                normed[b, pl.ds(pl.multiple_of(base + i * step_rows, step_rows), step_rows), :] = scaled[:, b * block : (b + 1) * block]
            return 0

        lax.fori_loop(0, tokens // step_rows, body, 0)

    with jax.named_scope("s_norm"):
        local[0].wait()
        norm_rows(first, 0)
        local[1].wait()
        norm_rows(second, tokens)
    gacc[...] = jnp.zeros_like(gacc)
    uacc[...] = jnp.zeros_like(uacc)
    hgrad[...] = jnp.zeros_like(hgrad)

    experts = router_w.shape[0]
    top = picks_a.shape[1]
    local[2].wait()
    logits = jnp.zeros((experts, 2 * tokens), F32)
    for b in range(d_model // block):
        logits = logits + exact_dot(router_w[:, b * block : (b + 1) * block], normed[b], NT)
    affinity = sigmoid(logits)
    aff[...] = affinity
    labels = lax.broadcasted_iota(jnp.int32, (experts, tokens), 0)

    def picked(picks, affinities, k):
        hit = picks[0, k] == labels
        return jnp.sum(jnp.where(hit, affinities, 0.0), axis=0, keepdims=True), hit

    stats = []
    for m, picks in enumerate((picks_a, picks_b)):
        part = affinity[:, m * tokens : (m + 1) * tokens]
        tab = jnp.zeros((experts, tokens), F32)
        chosen = []
        for k in range(top):
            value, hit = picked(picks, part, k)
            chosen.append(value)
            tab = tab + jnp.where(hit, 1.0, 0.0)
        total = chosen[0]
        for value in chosen[1:]:
            total = total + value
        all_aff = jnp.sum(part, axis=0, keepdims=True)
        if m == 0:
            for k in range(top):
                routing_out[0, k] = ROUTE_SCALE * chosen[k] / total
        else:
            csum[...] = total
            spread[...] = all_aff
        stats.append((tab, part / all_aff))
    ones = jnp.ones((8, tokens), F32)
    counts_row = dot(ones, jnp.concatenate([stats[0][0], stats[1][0]], axis=0), NT, HIGH)
    shares_row = dot(ones, jnp.concatenate([stats[0][1], stats[1][1]], axis=0), NT, HIGH)
    row_id = lax.broadcasted_iota(jnp.int32, (8, 2 * experts), 0)
    packed = jnp.where(row_id == 0, counts_row, jnp.where(row_id == 1, shares_row, 0.0))
    cnt_src[...] = packed
    for copy in local[3:]:
        copy.wait()
    with jax.named_scope("s_barrier"):
        pl.semaphore_wait(barrier, 3 + 2 * NZ - 1 + NY - 2)

    for r in range(1, 2 * NZ):
        remote(cnt_src, cnt.at[r], csend.at[r], crecv.at[r], c_peer(r)).start()
    for m in range(4):
        z_copy(z_ref(G, 0, m, c, sgn), m).start()

    @pl.when(is_last)
    def _():
        for place in range(Y_START):
            y_copy(y_ref(*Y_ORDER[place], c, sgn, send_half), place).start()

    back = remote(upstream, returned, xsem.at[0], xsem.at[1], x_prev)
    back.start()

    half_e = experts // 2
    own_half = pl.ds(pl.multiple_of(c * half_e, half_e), half_e)
    other_half = pl.ds(pl.multiple_of((1 - c) * half_e, half_e), half_e)

    def cols(i, width):
        return pl.ds(pl.multiple_of(i * width, width), width)

    def rs_pair():
        return remote(rp.at[other_half, :], b0, rsend.at[0], rrecv.at[0], partner)

    def part(i):
        return r0.at[:, cols((z + sgn * (i + 1) + 2 * NZ) % NZ, block)]

    def ring(i, source):
        return remote(source, b1.at[i], rsend.at[1 + i], rrecv.at[1 + i], z_prev)

    def tile(yy):
        return (cols(yy // 2, 8), cols(yy % 2, 128))

    def rs_y(r):
        return remote(r1.at[tile((y + r) % NY)], b2.at[r], rsend.at[8 + r], rrecv.at[8 + r], y_peer(r))

    def ag_y(r):
        return remote(r2, r3.at[tile(y)], rsend.at[16 + r], rrecv.at[16 + r], y_peer(r))

    def ag_z(r):
        return remote(
            r3, router_grad.at[own_half, cols(z, block)], rsend.at[24 + r], rrecv.at[24 + r], z_peer(r)
        )

    def ag_pair():
        return remote(
            router_grad.at[own_half, :], router_grad.at[own_half, :], rsend.at[32], rrecv.at[32], partner
        )

    def router_0():
        for r in range(1, 2 * NZ):
            remote(cnt_src, cnt.at[r], csend.at[r], crecv.at[r], c_peer(r)).wait_recv()
        totals = cnt_src[...]
        for r in range(1, 2 * NZ):
            totals = totals + cnt[r]
        scale = experts / (top * length)
        frac = scale * totals[0:1, :]
        terms = frac * totals[1:2, :] / length
        lane = lax.broadcasted_iota(jnp.int32, (1, 2 * experts), 1)
        bal_a = jnp.sum(jnp.where(lane < experts, terms, 0.0), axis=1, keepdims=True)
        bal_b = jnp.sum(jnp.where(lane >= experts, terms, 0.0), axis=1, keepdims=True)
        balance_out[0] = jnp.where(lane == 0, bal_a, bal_b)[:, 0:2]
        e_sub = lax.broadcasted_iota(jnp.int32, (experts, 2 * experts), 0)
        e_lane = lax.broadcasted_iota(jnp.int32, (experts, 2 * experts), 1)
        frac_col = jnp.sum(jnp.where(e_lane == e_sub + experts, frac, 0.0), axis=1, keepdims=True)
        aff_b = aff[:, tokens : 2 * tokens]
        chosen_sum = csum[...]
        shares = aff_b / spread[...]
        inner = jnp.zeros((1, tokens), F32)
        for k in range(top):
            value, _ = picked(picks_b, aff_b, k)
            inner = inner + grads[0, k] * value
        agrad = jnp.zeros((experts, tokens), F32)
        for k in range(top):
            hit = picks_b[0, k] == labels
            cgrad = ROUTE_SCALE * (grads[0, k] / chosen_sum - inner / (chosen_sum * chosen_sum))
            agrad = agrad + jnp.where(hit, cgrad, 0.0)
        share_grad = frac_col / length
        agrad = agrad + (share_grad - jnp.sum(share_grad * shares, axis=0, keepdims=True)) / spread[...]
        lg = agrad * aff_b * (1.0 - aff_b)
        logit[...] = lg
        for b in range(d_model // block):
            rp[:, b * block : (b + 1) * block] = exact_dot(lg, normed[b, tokens : 2 * tokens, :], NN)
        rs_pair().start()

    def router_term():
        lg_t = jnp.transpose(logit[...])
        for b in range(d_model // block):
            at = slice(b * block, (b + 1) * block)
            qbuf[b] = dot(lg_t, router_w[:, at], NN, HIGH)

    def router_1():
        rs_pair().wait_recv()
        r0[...] = rp[own_half, :] + b0[...]
        ring(0, part(0)).start()

    def ring_step(i):
        ring(i - 1, b1.at[i - 1]).wait_recv()
        b1[i - 1] = b1[i - 1] + part(i)[...]

        @pl.when(i < NZ - 1)
        def _():
            ring(i, b1.at[i - 1]).start()

        @pl.when(i == NZ - 1)
        def _():
            r1[...] = b1[i - 1]
            for r in range(1, NY):
                rs_y(r).start()

    def router_3():
        for r in range(1, NY):
            rs_y(r).wait_recv()
        acc = r1[tile(y)]
        for r in range(1, NY):
            acc = acc + b2[r]
        r2[...] = acc
        r3[tile(y)] = acc
        for r in range(1, NY):
            ag_y(r).start()

    def router_4():
        for r in range(1, NY):
            ag_y(r).wait_recv()
        pltpu.make_async_copy(r3, router_grad.at[own_half, cols(z, block)], local_sem.at[1]).start()
        for r in range(1, NZ):
            ag_z(r).start()

    def router_5():
        for r in range(1, NZ):
            ag_z(r).wait_recv()
        pltpu.make_async_copy(r3, router_grad.at[own_half, cols(z, block)], local_sem.at[1]).wait()
        ag_pair().start()

    router_at = {4: router_0, 5: router_1, 7: router_term, 23: router_3, 26: router_4, 32: router_5}
    ring_at, ring_every = 5, 2

    n_tile = 256

    def z_rows(zz):
        return pl.ds(pl.multiple_of(zz * block, block), block)

    def g_block(zz):
        lhs = normed[zz]
        for n in range(hidden // n_tile):
            at = slice(n * n_tile, (n + 1) * n_tile)
            gacc[:, at] += dot(lhs, wgu[0, z_rows(zz), at])
            uacc[:, at] += dot(lhs, wgu[1, z_rows(zz), at])

    def make_hidden():
        def body(i, _):
            rows = cols(i, 16)
            v = gacc[rows, :]
            hid[rows, :] = (v * sigmoid(v) * uacc[rows, :]).astype(BF16)
            return 0

        lax.fori_loop(0, tokens // 16, body, 0)

    def out_send(zz):
        return remote(
            out.at[:, z_rows(zz)], arrived.at[:, z_rows(zz)], osend.at[zz], orecv.at[zz], x_next
        )

    def out_block(zz):
        acc = dot(hid[...], wd[:, z_rows(zz)])
        out[:, z_rows(zz)] = (first[:, z_rows(zz)].astype(F32) + acc).astype(BF16)
        out_send(zz).start()

    def hgrad_block(zz):
        lhs = returned[:, z_rows(zz)]
        for n in range(hidden // n_tile):
            at = slice(n * n_tile, (n + 1) * n_tile)
            hgrad[:, at] += dot(lhs, wd[at, z_rows(zz)], NT)

    def pair(fn, group):
        fn((z + group) % NZ)
        fn((z - group + NZ) % NZ)

    def on_g(q):
        @pl.when(q == 0)
        def _():
            g_block(z)

        @pl.when((q % 2 == 0) & (q > 0))
        def _():
            pair(g_block, q // 2)

        @pl.when(q == NZ - 1)
        def _():
            g_block((z + 4) % NZ)
            make_hidden()

            def body(i, _):
                out_block((z + i + NZ - 2) % NZ)
                return 0

            lax.fori_loop(0, 5, body, 0)

    def on_d(q):
        @pl.when(q == 0)
        def _():
            back.wait_recv()
            hgrad_block(z)

        @pl.when((q % 2 == 0) & (q > 0))
        def _():
            pair(hgrad_block, q // 2)

        @pl.when(q == 6)
        def _():
            pair(out_block, 3)

        @pl.when(q == NZ - 1)
        def _():
            out_block((z + 4) % NZ)
            hgrad_block((z + 4) % NZ)

    z_codes = [code(*entry) for entry in Z_ORDER]
    y_codes = [code(*entry) for entry in Y_ORDER]
    z_follow = [z_next_place(entry) for entry in Z_ORDER]
    d1 = Z_ORDER.index((D, 1, 0))
    g2_end = 3

    def by_kind(entry, fn):
        for kind in (G, D):

            @pl.when(entry // 64 == kind)
            def _():
                fn(kind, (entry % 64) // 4, entry % 4)

    def slot(t, _):
        nz = t - 1

        @pl.when((nz >= 0) & (nz < NZP))
        def _():
            follow = lookup(z_follow, nz)

            def arrived_z(kind, k, m):
                ref = z_ref(kind, k, m, c, sgn)
                with jax.named_scope("w_z"):
                    z_copy(ref, nz).wait_recv()

                @pl.when(follow >= 0)
                def _():
                    z_copy(ref, follow).start()

                dz_copy(ref, nz).start()

            by_kind(lookup(z_codes, nz), arrived_z)

            @pl.when(nz == g2_end)
            def _():
                for m in range(2):
                    z_copy(z_ref(D, 0, m, c, sgn), d1 + m).start()

        ndz = t - 2

        @pl.when((ndz >= 0) & (ndz < NZP))
        def _():
            def arrived_dz(kind, k, m):
                with jax.named_scope("w_dz"):
                    dz_copy(z_ref(kind, k, m, 1 - c, -sgn), ndz).wait_recv()

            by_kind(lookup(z_codes, ndz), arrived_dz)

        nyr = t - LA - LB * hops

        @pl.when((nyr >= 0) & (nyr < NYP))
        def _():
            def arrived_y(kind, q, m):
                ref = y_ref(kind, q, m, c, sgn, 1 - h)
                with jax.named_scope("w_y"):
                    y_copy(ref, nyr).wait_recv()

                @pl.when(jnp.logical_not(is_last))
                def _():
                    y_copy(ref, nyr).start()

                dy_copy(ref, nyr).start()

            by_kind(lookup(y_codes, nyr), arrived_y)

        nys = t + 1

        @pl.when(is_last & (nys >= Y_START) & (nys < NYP))
        def _():
            def inject(kind, q, m):
                y_copy(y_ref(kind, q, m, c, sgn, h), nys).start()

            by_kind(lookup(y_codes, nys), inject)

        nyd = t - LA - LB * hops_max - 1

        @pl.when((nyd >= 0) & (nyd < NYP))
        def _():
            def arrived_dy(kind, q, m):
                with jax.named_scope("w_dy"):
                    dy_copy(y_ref(kind, q, m, 1 - c, -sgn, 1 - h), nyd).wait_recv()
                if kind == G:

                    @pl.when(m == 1)
                    def _():
                        with jax.named_scope("c_g"):
                            on_g(q)

                else:
                    with jax.named_scope("c_d"):
                        on_d(q)

            by_kind(lookup(y_codes, nyd), arrived_dy)

        ring_i = (t - ring_at) // ring_every

        @pl.when((t > ring_at) & ((t - ring_at) % ring_every == 0) & (ring_i < NZ))
        def _():
            with jax.named_scope("ring_step"):
                ring_step(ring_i)

        for at, stage in router_at.items():

            @pl.when(t == at)
            def _():
                with jax.named_scope(stage.__name__):
                    stage()

        return 0

    lax.fori_loop(0, NYP + LA + LB * 4 + 1, slot, 0)

    def shared_back(i, _):
        rows = cols(i, 16)
        b_rows = pl.ds(pl.multiple_of(tokens + i * 16, 16), 16)
        v, u, hg = gacc[b_rows, :], uacc[b_rows, :], hgrad[rows, :]
        s = sigmoid(v)
        gg[rows, :] = (hg * u * (s * (1.0 + v * (1.0 - s)))).astype(BF16)
        ug[rows, :] = (hg * v * s).astype(BF16)
        return 0

    with jax.named_scope("t_back"):
        lax.fori_loop(0, tokens // 16, shared_back, 0)
    def grad_block(b, mean):
        at = z_rows(b)
        grad = dot(gg[...], wgu[0, at, :], NT) + dot(ug[...], wgu[1, at, :], NT)
        q = (grad + qbuf[b]) * gain[:, at]
        qbuf[b] = q
        return mean + jnp.sum(q * second[:, at].astype(F32), axis=-1, keepdims=True)

    with jax.named_scope("t_grad"):
        mean = lax.fori_loop(0, d_model // block, grad_block, jnp.zeros((tokens, 1), F32)) / d_model
    inv_b = inverse[tokens : 2 * tokens, 0:1]
    factor = inv_b * inv_b * mean

    def final_block(b, _):
        at = z_rows(b)
        values = second[:, at].astype(F32)
        part = inv_b * (qbuf[b] - values * factor)
        grad_out[:, at] = (returned[:, at].astype(F32) + part).astype(BF16)
        return 0

    with jax.named_scope("t_final"):
        lax.fori_loop(0, d_model // block, final_block, 0)

    with jax.named_scope("t_agpair"):
        ag_pair().wait_recv()
    results = [
        pltpu.make_async_copy(grad_out, input_grad, local_sem.at[0]),
        pltpu.make_async_copy(routing_out, routing, local_sem.at[2]),
        pltpu.make_async_copy(balance_out, balance, local_sem.at[3]),
    ]
    for result in results:
        result.start()

    def drain(count, body):
        def step(n, _):
            body(n)
            return 0

        lax.fori_loop(0, count, step, 0)

    with jax.named_scope("t_out"):
        drain(2 * NZ // 2, lambda n: out_send(n).wait())
    for order, copies in ((Z_ORDER, (z_copy, dz_copy)), (Y_ORDER, (y_copy, dy_copy))):
        for place, entry in enumerate(order):
            ref = g_piece(0, 0) if entry[0] == G else d_piece(0, 0)
            for copy in copies:
                copy(ref, place).wait_send()
    back.wait_send()
    for r in range(1, 2 * NZ):
        remote(cnt_src, cnt.at[r], csend.at[r], crecv.at[r], c_peer(r)).wait_send()
    rs_pair().wait_send()
    ag_pair().wait_send()
    for r in range(1, NZ):
        ring(r - 1, b1.at[0]).wait_send()
        ag_z(r).wait_send()
    for r in range(1, NY):
        rs_y(r).wait_send()
        ag_y(r).wait_send()
    for result in results:
        result.wait()


def leave(*refs):
    n = (len(refs) - 1) // 3
    sems = refs[-1]
    into = [pltpu.make_async_copy(refs[i], refs[2 * n + i], sems.at[0, i]) for i in range(n)]
    away = [pltpu.make_async_copy(refs[2 * n + i], refs[n + i], sems.at[1, i]) for i in range(n)]
    for copy in into:
        copy.start()
    for i in range(n):
        into[i].wait()
        away[i].start()
    for copy in away:
        copy.wait()


def shards(
    first_input, second_input, upstream, first_picks, second_picks, gate_grads,
    norm_gain, router_weight, gate_weight, up_weight, down_weight,
):
    tokens, d_model = first_input.shape[2:]
    hidden = gate_weight.shape[2]
    experts = router_weight.shape[1]
    top = first_picks.shape[3]
    block = d_model // NZ
    blocks = d_model // block
    vmem = pl.BlockSpec(memory_space=pltpu.VMEM)
    hbm = pl.BlockSpec(memory_space=pltpu.HBM)
    anywhere = pl.BlockSpec(memory_space=pl.ANY)
    sem = pltpu.SemaphoreType.DMA
    half = experts // 2
    outs = pl.pallas_call(
        kernel,
        out_shape=(
            jax.ShapeDtypeStruct((tokens, d_model), BF16),
            jax.ShapeDtypeStruct((1, top, 1, tokens), F32),
            jax.ShapeDtypeStruct((tokens, d_model), BF16),
            jax.ShapeDtypeStruct((experts, d_model), F32),
            jax.ShapeDtypeStruct((1, 1, 2), F32),
        ),
        in_specs=[hbm, hbm, hbm, vmem, vmem, vmem, vmem, hbm, hbm, hbm, hbm],
        out_specs=(anywhere,) * 5,
        scratch_shapes=[
            pltpu.VMEM((tokens, d_model), BF16),
            pltpu.VMEM((tokens, d_model), BF16),
            pltpu.VMEM((experts, d_model), F32),
            pltpu.VMEM((tokens, d_model), BF16),
            pltpu.VMEM((1, top, 1, tokens), F32),
            pltpu.VMEM((1, 1, 2), F32),
            pltpu.VMEM((2, d_model, hidden), BF16),
            pltpu.VMEM((hidden, d_model), BF16),
            pltpu.VMEM((tokens, d_model), BF16),
            pltpu.VMEM((blocks, 2 * tokens, block), BF16),
            pltpu.VMEM((2 * tokens, 128), F32),
            pltpu.VMEM((2 * tokens, hidden), F32),
            pltpu.VMEM((2 * tokens, hidden), F32),
            pltpu.VMEM((tokens, hidden), F32),
            pltpu.VMEM((tokens, hidden), BF16),
            pltpu.VMEM((tokens, hidden), BF16),
            pltpu.VMEM((tokens, hidden), BF16),
            pltpu.VMEM((tokens, d_model), BF16),
            pltpu.VMEM((blocks, tokens, block), F32),
            pltpu.VMEM((8, 2 * experts), F32),
            pltpu.VMEM((2 * NZ, 8, 2 * experts), F32),
            pltpu.VMEM((experts, 2 * tokens), F32),
            pltpu.VMEM((1, tokens), F32),
            pltpu.VMEM((1, tokens), F32),
            pltpu.VMEM((experts, tokens), F32),
            pltpu.VMEM((experts, d_model), F32),
            pltpu.VMEM((half, d_model), F32),
            pltpu.VMEM((half, d_model), F32),
            pltpu.VMEM((NZ, half, block), F32),
            pltpu.VMEM((half, block), F32),
            pltpu.VMEM((NY, 8, 128), F32),
            pltpu.VMEM((8, 128), F32),
            pltpu.VMEM((half, block), F32),
            sem((6,)),
            sem((NZP,)), sem((NZP,)), sem((NYP,)), sem((NYP,)),
            sem((NZP,)), sem((NZP,)), sem((NYP,)), sem((NYP,)),
            sem((2,)), sem((NZ,)), sem((NZ,)),
            sem((2 * NZ,)), sem((2 * NZ,)), sem((33,)), sem((33,)),
        ],
        compiler_params=pltpu.CompilerParams(
            collective_id=0, has_side_effects=True, vmem_limit_bytes=62 * 1024 * 1024
        ),
    )(
        first_input[0, 0],
        second_input[0, 0],
        upstream[0, 0],
        jnp.transpose(first_picks, (0, 3, 1, 2)),
        jnp.transpose(second_picks, (0, 3, 1, 2)),
        jnp.transpose(gate_grads, (0, 3, 1, 2)),
        norm_gain,
        router_weight[0],
        gate_weight[0],
        up_weight[0],
        down_weight[0],
    )
    arrived, routing, input_grad, router_grad, balance = pl.pallas_call(
        leave,
        out_shape=tuple(jax.ShapeDtypeStruct(a.shape, a.dtype) for a in outs),
        in_specs=[anywhere] * 5,
        out_specs=(hbm,) * 5,
        scratch_shapes=[pltpu.VMEM(a.shape, a.dtype) for a in outs] + [sem((2, 5))],
    )(*outs)
    return (
        arrived[None, None],
        jnp.transpose(routing, (0, 2, 3, 1)),
        input_grad[None, None],
        router_grad[None],
        balance,
    )


def solution(mesh):
    split = Mesh(
        mesh.devices.reshape(mesh.shape["section"], NZ, 2, mesh.shape["dp"]),
        ("section", "ctx_0", "ctx_1", "dp"),
    )
    tokens = P("section", "dp", CTX, None)
    return jax.shard_map(
        shards,
        mesh=split,
        in_specs=(tokens,) * 6
        + (
            P("section", None),
            P("section", None, None),
            P("section", CTX, None),
            P("section", CTX, None),
            P("section", None, CTX),
        ),
        out_specs=(tokens,) * 3 + (P("section", None, None), P("section", "dp", None)),
        check_vma=False,
    )
```

```python
import jax
import jax.numpy as jnp
from jax import lax
from jax.experimental import pallas as pl
from jax.experimental.pallas import tpu as pltpu
from jax.sharding import Mesh
from jax.sharding import PartitionSpec as P

CTX = ("ctx_0", "ctx_1")
MESH = pl.DeviceIdType.MESH
EPSILON = 1e-06
ROUTE_SCALE = 2.5
HIGH = lax.Precision.HIGHEST
F32 = jnp.float32
BF16 = jnp.bfloat16

NZ, NY, NX = 8, 8, 4
G, D = 0, 1
Z_ORDER = (
    [(G, 1, m) for m in range(4)]
    + [(G, 2, m) for m in range(4)]
    + [(D, 1, m) for m in range(2)]
    + [(G, 3, m) for m in range(4)]
    + [(D, 2, m) for m in range(2)]
    + [(G, 4, m) for m in range(2)]
    + [(D, 3, m) for m in range(2)]
    + [(D, 4, 0)]
)
Y_ORDER = [(G, 0, 0), (G, 0, 1), (D, 0, 0)]
for _q in ((G, 1), (G, 2), (G, 3), (G, 4), (D, 1), (D, 2), (G, 5), (G, 6), (D, 3), (D, 4)):
    Y_ORDER += [(_q[0], _q[1], m) for m in range(2 - _q[0])]
NZP, NYP = len(Z_ORDER), len(Y_ORDER)
E_ORDER = [(G, 4, 0), (G, 4, 0), (D, 3, 0), (D, 3, 1), (D, 4, 0)]
NE = len(E_ORDER)
G5, D3, D4 = Y_ORDER.index((G, 5, 0)), Y_ORDER.index((D, 3, 0)), Y_ORDER.index((D, 4, 0))
E_LAG = 2
Y_START = 3
LA, LB = 1, 2


def lookup(values, i):
    out = jnp.int32(values[0])
    for p in range(1, len(values)):
        if values[p] != values[p - 1]:
            out = jnp.where(i >= p, jnp.int32(values[p]), out)
    return out


def code(kind, k, m):
    return kind * 64 + k * 4 + m


def z_next_place(entry):
    kind, k, m = entry
    return Z_ORDER.index((kind, k + 1, m)) if (kind, k + 1, m) in Z_ORDER else -1

NT = (((1,), (1,)), ((), ()))
TN = (((0,), (0,)), ((), ()))
NN = (((1,), (0,)), ((), ()))


def dot(a, b, dims=NN, precision=None):
    return lax.dot_general(a, b, dims, precision=precision, preferred_element_type=F32)


def exact_dot(a, b, dims):
    rows = a.shape[0]
    one = a.astype(BF16)
    left = a - one.astype(F32)
    two = left.astype(BF16)
    three = (left - two.astype(F32)).astype(BF16)
    parts = dot(jnp.concatenate([one, two, three], axis=0), b, dims)
    return parts[2 * rows :] + parts[rows : 2 * rows] + parts[:rows]


def sigmoid(v):
    return jax.nn.sigmoid(v)


def kernel(
    first_hbm, second_hbm, upstream, picks_a, picks_b, grads, gain, router_hbm, gate, up, down,
    arrived, routing, input_grad, router_grad, balance,
    first, second, router_w, grad_out, routing_out, balance_out, wgu, wd, returned, normed, inverse, gacc, uacc, hgrad, hid, gg, ug, out, qbuf,
    cnt_src, cnt, aff, csum, spread, logit,
    rp, r0, b0, b1, r1, b2, r2, r3,
    local_sem, zsend, zrecv, ysend, yrecv, dzsend, dzrecv, dysend, dyrecv,
    xsem, osend, orecv, csend, crecv, rsend, rrecv,
):
    d_model = gate.shape[0] * 2 * NZ
    hidden = gate.shape[1]
    tokens = first_hbm.shape[0]
    rows_s = gate.shape[0]
    pg, pd = rows_s // 4, hidden // 2
    block = 2 * rows_s
    length = tokens * 2 * NZ

    x = lax.axis_index("section")
    z = lax.axis_index("ctx_0")
    h = lax.axis_index("ctx_1")
    dp = lax.axis_index("dp")
    j = dp // 2
    c = dp % 2
    y = h * 4 + j
    sgn = 1 - 2 * c

    def dev(xx, zz, yy, cc):
        return (xx, zz, yy // 4, (yy % 4) * 2 + cc)

    partner = dev(x, z, y, 1 - c)
    z_next = dev(x, (z + sgn + NZ) % NZ, y, c)
    y_prev = dev(x, z, (y - sgn + NY) % NY, c)
    y_next = dev(x, z, (y + sgn + NY) % NY, c)
    x_next = dev((x + 1) % NX, z, y, c)
    x_prev = dev((x + NX - 1) % NX, z, y, c)

    def z_peer(r):
        return dev(x, (z + r) % NZ, y, c)

    def y_peer(r):
        return dev(x, z, (y + r) % NY, c)

    def c_peer(r):
        rank = (z * 2 + h + r) % (2 * NZ)
        return (x, rank // 2, rank % 2, dp)

    def remote(src, dst, send, recv, device):
        return pltpu.make_async_remote_copy(
            src_ref=src, dst_ref=dst, send_sem=send, recv_sem=recv, device_id=device, device_id_type=MESH
        )

    barrier = pltpu.get_barrier_semaphore()

    def greet(device):
        pl.semaphore_signal(barrier, inc=1, device_id=device, device_id_type=MESH)

    greet(partner)
    greet(x_next)
    greet(x_prev)
    for r in range(1, 2 * NZ):
        greet(c_peer(r))
    for r in range(1, NY):
        if r != 4:
            greet(y_peer(r))

    own = z * 2 + h
    own_rows = pl.ds(pl.multiple_of(own * rows_s, rows_s), rows_s)
    local = [
        pltpu.make_async_copy(first_hbm, first, local_sem.at[0]),
        pltpu.make_async_copy(second_hbm, second, local_sem.at[1]),
        pltpu.make_async_copy(router_hbm, router_w, local_sem.at[2]),
        pltpu.make_async_copy(gate, wgu.at[0, own_rows, :], local_sem.at[3]),
        pltpu.make_async_copy(up, wgu.at[1, own_rows, :], local_sem.at[4]),
        pltpu.make_async_copy(down, wd.at[:, own_rows], local_sem.at[5]),
    ]
    for copy in local:
        copy.start()

    def g_piece(slot, p):
        start = pl.multiple_of(slot * rows_s + p * pg, pg)
        return wgu.at[:, pl.ds(start, pg), :]

    def d_piece(slot, p):
        return wd.at[pl.ds(pl.multiple_of(p * pd, pd), pd), pl.ds(pl.multiple_of(slot * rows_s, rows_s), rows_s)]

    def slot_of(zz, hh):
        return ((zz + 2 * NZ) % NZ) * 2 + hh

    def z_ref(kind, k, m, core, sign):
        slot = slot_of(z - sign * k, h)
        if kind == G:
            return g_piece(slot, (2 * core + m) % 4)
        return d_piece(slot, (core + m) % 2)

    def y_ref(kind, q, m, core, sign, hh):
        slot = slot_of(z + (1 - 2 * (q % 2)) * ((q + 1) // 2) * sign, hh)
        if kind == G:
            return g_piece(slot, 2 * core + m)
        return d_piece(slot, core)

    def e_ref(i, core, sign):
        kind, k, flip = E_ORDER[i]
        slot = slot_of(z - sign * k, 1 - h)
        if kind == G:
            return g_piece(slot, 2 * core + i)
        return d_piece(slot, (core + flip) % 2)

    def z_copy(ref, place):
        return remote(ref, ref, zsend.at[place], zrecv.at[place], z_next)

    def y_copy(ref, place):
        return remote(ref, ref, ysend.at[place], yrecv.at[place], y_next)

    def dz_copy(ref, place):
        return remote(ref, ref, dzsend.at[place], dzrecv.at[place], partner)

    def dy_copy(ref, place):
        return remote(ref, ref, dysend.at[place], dyrecv.at[place], partner)

    last = 3 * (1 - c)
    is_last = j == last
    hops = jnp.where(c == 0, j + 1, 4 - j)
    hops_max = jnp.maximum(hops, 5 - hops)
    send_half = jnp.where(is_last, h, 1 - h)

    step_rows = 16

    def norm_rows(source, base):
        def body(i, _):
            rows = pl.ds(pl.multiple_of(i * step_rows, step_rows), step_rows)
            values = source[rows, :].astype(F32)
            inv = lax.rsqrt(jnp.mean(values * values, axis=-1, keepdims=True) + EPSILON)
            inverse[pl.ds(pl.multiple_of(base + i * step_rows, step_rows), step_rows), :] = jnp.broadcast_to(inv, (step_rows, 128))
            scaled = (values * inv * gain[...]).astype(BF16)
            for b in range(d_model // block):
                normed[b, pl.ds(pl.multiple_of(base + i * step_rows, step_rows), step_rows), :] = scaled[:, b * block : (b + 1) * block]
            return 0

        lax.fori_loop(0, tokens // step_rows, body, 0)

    with jax.named_scope("s_norm"):
        local[0].wait()
        norm_rows(first, 0)
        local[1].wait()
        norm_rows(second, tokens)
    gacc[...] = jnp.zeros_like(gacc)
    uacc[...] = jnp.zeros_like(uacc)
    hgrad[...] = jnp.zeros_like(hgrad)

    experts = router_w.shape[0]
    top = picks_a.shape[1]
    local[2].wait()
    logits = jnp.zeros((experts, 2 * tokens), F32)
    for b in range(d_model // block):
        logits = logits + exact_dot(router_w[:, b * block : (b + 1) * block], normed[b], NT)
    affinity = sigmoid(logits)
    aff[...] = affinity
    labels = lax.broadcasted_iota(jnp.int32, (experts, tokens), 0)

    def picked(picks, affinities, k):
        hit = picks[0, k] == labels
        return jnp.sum(jnp.where(hit, affinities, 0.0), axis=0, keepdims=True), hit

    stats = []
    for m, picks in enumerate((picks_a, picks_b)):
        part = affinity[:, m * tokens : (m + 1) * tokens]
        tab = jnp.zeros((experts, tokens), F32)
        chosen = []
        for k in range(top):
            value, hit = picked(picks, part, k)
            chosen.append(value)
            tab = tab + jnp.where(hit, 1.0, 0.0)
        total = chosen[0]
        for value in chosen[1:]:
            total = total + value
        all_aff = jnp.sum(part, axis=0, keepdims=True)
        if m == 0:
            for k in range(top):
                routing_out[0, k] = ROUTE_SCALE * chosen[k] / total
        else:
            csum[...] = total
            spread[...] = all_aff
        stats.append((tab, part / all_aff))
    ones = jnp.ones((8, tokens), F32)
    counts_row = dot(ones, jnp.concatenate([stats[0][0], stats[1][0]], axis=0), NT, HIGH)
    shares_row = dot(ones, jnp.concatenate([stats[0][1], stats[1][1]], axis=0), NT, HIGH)
    row_id = lax.broadcasted_iota(jnp.int32, (8, 2 * experts), 0)
    packed = jnp.where(row_id == 0, counts_row, jnp.where(row_id == 1, shares_row, 0.0))
    cnt_src[...] = packed
    for copy in local[3:]:
        copy.wait()
    with jax.named_scope("s_barrier"):
        pl.semaphore_wait(barrier, 3 + 2 * NZ - 1 + NY - 2)

    for r in range(1, 2 * NZ):
        remote(cnt_src, cnt.at[r], csend.at[r], crecv.at[r], c_peer(r)).start()
    for m in range(4):
        z_copy(z_ref(G, 0, m, c, sgn), m).start()

    @pl.when(is_last)
    def _():
        for place in range(Y_START):
            y_copy(y_ref(*Y_ORDER[place], c, sgn, send_half), place).start()

    back = remote(upstream, returned, xsem.at[0], xsem.at[1], x_prev)
    back.start()

    half_e = experts // 2
    own_half = pl.ds(pl.multiple_of(c * half_e, half_e), half_e)
    other_half = pl.ds(pl.multiple_of((1 - c) * half_e, half_e), half_e)

    def cols(i, width):
        return pl.ds(pl.multiple_of(i * width, width), width)

    def rs_pair():
        return remote(rp.at[other_half, :], b0, rsend.at[0], rrecv.at[0], partner)

    def part(i):
        return r0.at[:, cols((y + sgn * (i + 1) + 2 * NY) % NY, block)]

    def ring(i, source):
        return remote(source, b1.at[i], rsend.at[1 + i], rrecv.at[1 + i], y_prev)

    def tile(yy):
        return (cols(yy // 2, 8), cols(yy % 2, 128))

    def rs_small(r):
        return remote(r1.at[tile((z + r) % NZ)], b2.at[r], rsend.at[8 + r], rrecv.at[8 + r], z_peer(r))

    def ag_small(r):
        return remote(r2, r3.at[tile(z)], rsend.at[16 + r], rrecv.at[16 + r], z_peer(r))

    def ag_big(r):
        return remote(
            r3, router_grad.at[own_half, cols(y, block)], rsend.at[24 + r], rrecv.at[24 + r], y_peer(r)
        )

    def ag_pair():
        return remote(
            router_grad.at[own_half, :], router_grad.at[own_half, :], rsend.at[32], rrecv.at[32], partner
        )

    def router_0():
        for r in range(1, 2 * NZ):
            remote(cnt_src, cnt.at[r], csend.at[r], crecv.at[r], c_peer(r)).wait_recv()
        totals = cnt_src[...]
        for r in range(1, 2 * NZ):
            totals = totals + cnt[r]
        scale = experts / (top * length)
        frac = scale * totals[0:1, :]
        terms = frac * totals[1:2, :] / length
        lane = lax.broadcasted_iota(jnp.int32, (1, 2 * experts), 1)
        bal_a = jnp.sum(jnp.where(lane < experts, terms, 0.0), axis=1, keepdims=True)
        bal_b = jnp.sum(jnp.where(lane >= experts, terms, 0.0), axis=1, keepdims=True)
        balance_out[0] = jnp.where(lane == 0, bal_a, bal_b)[:, 0:2]
        e_sub = lax.broadcasted_iota(jnp.int32, (experts, 2 * experts), 0)
        e_lane = lax.broadcasted_iota(jnp.int32, (experts, 2 * experts), 1)
        frac_col = jnp.sum(jnp.where(e_lane == e_sub + experts, frac, 0.0), axis=1, keepdims=True)
        aff_b = aff[:, tokens : 2 * tokens]
        chosen_sum = csum[...]
        shares = aff_b / spread[...]
        inner = jnp.zeros((1, tokens), F32)
        for k in range(top):
            value, _ = picked(picks_b, aff_b, k)
            inner = inner + grads[0, k] * value
        agrad = jnp.zeros((experts, tokens), F32)
        for k in range(top):
            hit = picks_b[0, k] == labels
            cgrad = ROUTE_SCALE * (grads[0, k] / chosen_sum - inner / (chosen_sum * chosen_sum))
            agrad = agrad + jnp.where(hit, cgrad, 0.0)
        share_grad = frac_col / length
        agrad = agrad + (share_grad - jnp.sum(share_grad * shares, axis=0, keepdims=True)) / spread[...]
        lg = agrad * aff_b * (1.0 - aff_b)
        logit[...] = lg
        for b in range(d_model // block):
            rp[:, b * block : (b + 1) * block] = exact_dot(lg, normed[b, tokens : 2 * tokens, :], NN)
        rs_pair().start()

    def router_term():
        lg_t = jnp.transpose(logit[...])
        for b in range(d_model // block):
            at = slice(b * block, (b + 1) * block)
            qbuf[b] = dot(lg_t, router_w[:, at], NN, HIGH)

    def router_1():
        rs_pair().wait_recv()
        r0[...] = rp[own_half, :] + b0[...]
        ring(0, part(0)).start()

    def ring_step(i):
        ring(i - 1, b1.at[i - 1]).wait_recv()
        b1[i - 1] = b1[i - 1] + part(i)[...]

        @pl.when(i < NZ - 1)
        def _():
            ring(i, b1.at[i - 1]).start()

        @pl.when(i == NZ - 1)
        def _():
            r1[...] = b1[i - 1]
            for r in range(1, NY):
                rs_small(r).start()

    def router_3():
        for r in range(1, NY):
            rs_small(r).wait_recv()
        acc = r1[tile(z)]
        for r in range(1, NY):
            acc = acc + b2[r]
        r2[...] = acc
        r3[tile(z)] = acc
        for r in range(1, NY):
            ag_small(r).start()

    def router_4():
        for r in range(1, NY):
            ag_small(r).wait_recv()
        pltpu.make_async_copy(r3, router_grad.at[own_half, cols(y, block)], local_sem.at[1]).start()

    def router_5():
        for r in range(1, NZ):
            ag_big(r).wait_recv()
        pltpu.make_async_copy(r3, router_grad.at[own_half, cols(y, block)], local_sem.at[1]).wait()
        ag_pair().start()

    router_at = {4: router_0, 5: router_1, 7: router_term, 22: router_3, 25: router_4}
    ring_at, ring_every, spread_at = 5, 2, 25

    n_tile = 256

    def z_rows(zz):
        return pl.ds(pl.multiple_of(zz * block, block), block)

    def g_block(zz):
        lhs = normed[zz]
        for n in range(hidden // n_tile):
            at = slice(n * n_tile, (n + 1) * n_tile)
            gacc[:, at] += dot(lhs, wgu[0, z_rows(zz), at])
            uacc[:, at] += dot(lhs, wgu[1, z_rows(zz), at])

    def make_hidden():
        def body(i, _):
            rows = cols(i, 16)
            v = gacc[rows, :]
            hid[rows, :] = (v * sigmoid(v) * uacc[rows, :]).astype(BF16)
            return 0

        lax.fori_loop(0, tokens // 16, body, 0)

    def out_send(zz):
        return remote(
            out.at[:, z_rows(zz)], arrived.at[:, z_rows(zz)], osend.at[zz], orecv.at[zz], x_next
        )

    def out_block(zz):
        acc = dot(hid[...], wd[:, z_rows(zz)])
        out[:, z_rows(zz)] = (first[:, z_rows(zz)].astype(F32) + acc).astype(BF16)
        out_send(zz).start()

    def hgrad_block(zz):
        lhs = returned[:, z_rows(zz)]
        for n in range(hidden // n_tile):
            at = slice(n * n_tile, (n + 1) * n_tile)
            hgrad[:, at] += dot(lhs, wd[at, z_rows(zz)], NT)

    def pair(fn, group):
        fn((z + group) % NZ)
        fn((z - group + NZ) % NZ)

    def on_g(q):
        @pl.when(q == 0)
        def _():
            g_block(z)

        @pl.when((q % 2 == 0) & (q > 0))
        def _():
            pair(g_block, q // 2)

    def all_g():
        g_block((z + 4) % NZ)
        make_hidden()

        def body(i, _):
            out_block((z + i + NZ - 1) % NZ)
            return 0

        lax.fori_loop(0, 3, body, 0)

    def on_d(q):
        @pl.when(q == 0)
        def _():
            back.wait_recv()
            hgrad_block(z)

        @pl.when((q % 2 == 0) & (q > 0))
        def _():
            pair(hgrad_block, q // 2)

        @pl.when(q == 4)
        def _():
            pair(out_block, 2)

    def all_d():
        pair(hgrad_block, 3)
        hgrad_block((z + 4) % NZ)
        pair(out_block, 3)
        out_block((z + 4) % NZ)

    z_codes = [code(*entry) for entry in Z_ORDER]
    y_codes = [code(*entry) for entry in Y_ORDER]
    z_follow = [z_next_place(entry) for entry in Z_ORDER]
    d1 = Z_ORDER.index((D, 1, 0))
    g2_end = 3

    def by_kind(entry, fn):
        for kind in (G, D):

            @pl.when(entry // 64 == kind)
            def _():
                fn(kind, (entry % 64) // 4, entry % 4)

    def slot(t, _):
        nz = t - 1

        @pl.when((nz >= 0) & (nz < NZP))
        def _():
            follow = lookup(z_follow, nz)

            def arrived_z(kind, k, m):
                ref = z_ref(kind, k, m, c, sgn)
                with jax.named_scope("w_z"):
                    z_copy(ref, nz).wait_recv()

                @pl.when(follow >= 0)
                def _():
                    z_copy(ref, follow).start()

                dz_copy(ref, nz).start()

            by_kind(lookup(z_codes, nz), arrived_z)

            @pl.when(nz == g2_end)
            def _():
                for m in range(2):
                    z_copy(z_ref(D, 0, m, c, sgn), d1 + m).start()

        ndz = t - 2

        @pl.when((ndz >= 0) & (ndz < NZP))
        def _():
            def arrived_dz(kind, k, m):
                with jax.named_scope("w_dz"):
                    dz_copy(z_ref(kind, k, m, 1 - c, -sgn), ndz).wait_recv()

            by_kind(lookup(z_codes, ndz), arrived_dz)

        nyr = t - LA - LB * hops

        @pl.when((nyr >= 0) & (nyr < NYP))
        def _():
            def arrived_y(kind, q, m):
                ref = y_ref(kind, q, m, c, sgn, 1 - h)
                with jax.named_scope("w_y"):
                    y_copy(ref, nyr).wait_recv()

                @pl.when(jnp.logical_not(is_last))
                def _():
                    y_copy(ref, nyr).start()

                dy_copy(ref, nyr).start()
                if kind == G:

                    @pl.when(q == 5)
                    def _():
                        z_copy(ref, NZP + m).start()

                else:

                    @pl.when(q == 3)
                    def _():
                        z_copy(ref, NZP + 2).start()

            by_kind(lookup(y_codes, nyr), arrived_y)

        def arrived_e(i):
            ref = e_ref(i, c, sgn)
            with jax.named_scope("w_e"):
                z_copy(ref, NZP + i).wait_recv()
            if i == 2:
                z_copy(ref, NZP + 4).start()
            dz_copy(ref, NZP + i).start()

        def arrived_de(i):
            with jax.named_scope("w_de"):
                dz_copy(e_ref(i, 1 - c, -sgn), NZP + i).wait_recv()

        late = t - LA - LB * hops_max
        for i, place in ((0, G5), (1, G5 + 1), (2, D3), (4, D3 + E_LAG)):

            @pl.when(late == place + E_LAG)
            def _():
                arrived_e(i)

        nys = t + 1

        @pl.when(is_last & (nys >= Y_START) & (nys < NYP))
        def _():
            def inject(kind, q, m):
                y_copy(y_ref(kind, q, m, c, sgn, h), nys).start()

            by_kind(lookup(y_codes, nys), inject)

        nyd = t - LA - LB * hops_max - 1

        @pl.when((nyd >= 0) & (nyd < NYP))
        def _():
            def arrived_dy(kind, q, m):
                with jax.named_scope("w_dy"):
                    dy_copy(y_ref(kind, q, m, 1 - c, -sgn, 1 - h), nyd).wait_recv()
                if kind == G:

                    @pl.when(m == 1)
                    def _():
                        with jax.named_scope("c_g"):
                            on_g(q)

                else:
                    @pl.when(q == 4)
                    def _():
                        z_copy(y_ref(kind, q, m, 1 - c, -sgn, 1 - h), NZP + 3).start()

                    with jax.named_scope("c_d"):
                        on_d(q)

            by_kind(lookup(y_codes, nyd), arrived_dy)

        @pl.when(nyd == G5 + E_LAG)
        def _():
            arrived_de(0)

        @pl.when(nyd == G5 + 1 + E_LAG)
        def _():
            arrived_de(1)
            with jax.named_scope("c_allg"):
                all_g()

        @pl.when(nyd == D3 + E_LAG)
        def _():
            arrived_de(2)

        @pl.when(nyd == D4 + E_LAG)
        def _():
            arrived_e(3)

        @pl.when(nyd == D4 + E_LAG + 1)
        def _():
            arrived_de(3)
            arrived_de(4)
            with jax.named_scope("c_alld"):
                all_d()

        ring_i = (t - ring_at) // ring_every

        @pl.when((t > ring_at) & ((t - ring_at) % ring_every == 0) & (ring_i < NZ))
        def _():
            with jax.named_scope("ring_step"):
                ring_step(ring_i)

        for at, stage in router_at.items():

            @pl.when(t == at)
            def _():
                with jax.named_scope(stage.__name__):
                    stage()

        spread_i = t - spread_at

        @pl.when((spread_i >= 0) & (spread_i < 4))
        def _():
            ag_big(4 + spread_i).start()

            @pl.when(spread_i < 3)
            def _():
                ag_big(3 - spread_i).start()

        return 0

    lax.fori_loop(0, D4 + E_LAG + 2 + LA + LB * 4 + 1, slot, 0)

    def shared_back(i, _):
        rows = cols(i, 16)
        b_rows = pl.ds(pl.multiple_of(tokens + i * 16, 16), 16)
        v, u, hg = gacc[b_rows, :], uacc[b_rows, :], hgrad[rows, :]
        s = sigmoid(v)
        gg[rows, :] = (hg * u * (s * (1.0 + v * (1.0 - s)))).astype(BF16)
        ug[rows, :] = (hg * v * s).astype(BF16)
        return 0

    with jax.named_scope("t_back"):
        lax.fori_loop(0, tokens // 16, shared_back, 0)
    def grad_block(b, mean):
        at = z_rows(b)
        grad = dot(gg[...], wgu[0, at, :], NT) + dot(ug[...], wgu[1, at, :], NT)
        q = (grad + qbuf[b]) * gain[:, at]
        qbuf[b] = q
        return mean + jnp.sum(q * second[:, at].astype(F32), axis=-1, keepdims=True)

    with jax.named_scope("router_5"):
        router_5()
    with jax.named_scope("t_grad"):
        mean = lax.fori_loop(0, d_model // block, grad_block, jnp.zeros((tokens, 1), F32), unroll=True) / d_model
    inv_b = inverse[tokens : 2 * tokens, 0:1]
    factor = inv_b * inv_b * mean

    def final_block(b, _):
        at = z_rows(b)
        values = second[:, at].astype(F32)
        part = inv_b * (qbuf[b] - values * factor)
        grad_out[:, at] = (returned[:, at].astype(F32) + part).astype(BF16)
        return 0

    with jax.named_scope("t_final"):
        lax.fori_loop(0, d_model // block, final_block, 0)

    with jax.named_scope("t_agpair"):
        ag_pair().wait_recv()
    results = [
        pltpu.make_async_copy(grad_out, input_grad, local_sem.at[0]),
        pltpu.make_async_copy(routing_out, routing, local_sem.at[2]),
        pltpu.make_async_copy(balance_out, balance, local_sem.at[3]),
    ]
    for result in results:
        result.start()

    def drain(count, body):
        def step(n, _):
            body(n)
            return 0

        lax.fori_loop(0, count, step, 0)

    with jax.named_scope("t_out"):
        drain(2 * NZ // 2, lambda n: out_send(n).wait())
    for order, copies in ((Z_ORDER + E_ORDER, (z_copy, dz_copy)), (Y_ORDER, (y_copy, dy_copy))):
        for place, entry in enumerate(order):
            ref = g_piece(0, 0) if entry[0] == G else d_piece(0, 0)
            for copy in copies:
                copy(ref, place).wait_send()
    back.wait_send()
    for r in range(1, 2 * NZ):
        remote(cnt_src, cnt.at[r], csend.at[r], crecv.at[r], c_peer(r)).wait_send()
    rs_pair().wait_send()
    ag_pair().wait_send()
    for r in range(1, NZ):
        ring(r - 1, b1.at[0]).wait_send()
        ag_big(r).wait_send()
    for r in range(1, NY):
        rs_small(r).wait_send()
        ag_small(r).wait_send()
    for result in results:
        result.wait()


def leave(*refs):
    n = (len(refs) - 1) // 3
    sems = refs[-1]
    into = [pltpu.make_async_copy(refs[i], refs[2 * n + i], sems.at[0, i]) for i in range(n)]
    away = [pltpu.make_async_copy(refs[2 * n + i], refs[n + i], sems.at[1, i]) for i in range(n)]
    for copy in into:
        copy.start()
    for i in range(n):
        into[i].wait()
        away[i].start()
    for copy in away:
        copy.wait()


def shards(
    first_input, second_input, upstream, first_picks, second_picks, gate_grads,
    norm_gain, router_weight, gate_weight, up_weight, down_weight,
):
    tokens, d_model = first_input.shape[2:]
    hidden = gate_weight.shape[2]
    experts = router_weight.shape[1]
    top = first_picks.shape[3]
    block = d_model // NZ
    blocks = d_model // block
    vmem = pl.BlockSpec(memory_space=pltpu.VMEM)
    hbm = pl.BlockSpec(memory_space=pltpu.HBM)
    anywhere = pl.BlockSpec(memory_space=pl.ANY)
    sem = pltpu.SemaphoreType.DMA
    half = experts // 2
    outs = pl.pallas_call(
        kernel,
        out_shape=(
            jax.ShapeDtypeStruct((tokens, d_model), BF16),
            jax.ShapeDtypeStruct((1, top, 1, tokens), F32),
            jax.ShapeDtypeStruct((tokens, d_model), BF16),
            jax.ShapeDtypeStruct((experts, d_model), F32),
            jax.ShapeDtypeStruct((1, 1, 2), F32),
        ),
        in_specs=[hbm, hbm, hbm, vmem, vmem, vmem, vmem, hbm, hbm, hbm, hbm],
        out_specs=(anywhere,) * 5,
        scratch_shapes=[
            pltpu.VMEM((tokens, d_model), BF16),
            pltpu.VMEM((tokens, d_model), BF16),
            pltpu.VMEM((experts, d_model), F32),
            pltpu.VMEM((tokens, d_model), BF16),
            pltpu.VMEM((1, top, 1, tokens), F32),
            pltpu.VMEM((1, 1, 2), F32),
            pltpu.VMEM((2, d_model, hidden), BF16),
            pltpu.VMEM((hidden, d_model), BF16),
            pltpu.VMEM((tokens, d_model), BF16),
            pltpu.VMEM((blocks, 2 * tokens, block), BF16),
            pltpu.VMEM((2 * tokens, 128), F32),
            pltpu.VMEM((2 * tokens, hidden), F32),
            pltpu.VMEM((2 * tokens, hidden), F32),
            pltpu.VMEM((tokens, hidden), F32),
            pltpu.VMEM((tokens, hidden), BF16),
            pltpu.VMEM((tokens, hidden), BF16),
            pltpu.VMEM((tokens, hidden), BF16),
            pltpu.VMEM((tokens, d_model), BF16),
            pltpu.VMEM((blocks, tokens, block), F32),
            pltpu.VMEM((8, 2 * experts), F32),
            pltpu.VMEM((2 * NZ, 8, 2 * experts), F32),
            pltpu.VMEM((experts, 2 * tokens), F32),
            pltpu.VMEM((1, tokens), F32),
            pltpu.VMEM((1, tokens), F32),
            pltpu.VMEM((experts, tokens), F32),
            pltpu.VMEM((experts, d_model), F32),
            pltpu.VMEM((half, d_model), F32),
            pltpu.VMEM((half, d_model), F32),
            pltpu.VMEM((NZ, half, block), F32),
            pltpu.VMEM((half, block), F32),
            pltpu.VMEM((NY, 8, 128), F32),
            pltpu.VMEM((8, 128), F32),
            pltpu.VMEM((half, block), F32),
            sem((6,)),
            sem((NZP + NE,)), sem((NZP + NE,)), sem((NYP,)), sem((NYP,)),
            sem((NZP + NE,)), sem((NZP + NE,)), sem((NYP,)), sem((NYP,)),
            sem((2,)), sem((NZ,)), sem((NZ,)),
            sem((2 * NZ,)), sem((2 * NZ,)), sem((33,)), sem((33,)),
        ],
        compiler_params=pltpu.CompilerParams(
            collective_id=0, has_side_effects=True, vmem_limit_bytes=62 * 1024 * 1024
        ),
    )(
        first_input[0, 0],
        second_input[0, 0],
        upstream[0, 0],
        jnp.transpose(first_picks, (0, 3, 1, 2)),
        jnp.transpose(second_picks, (0, 3, 1, 2)),
        jnp.transpose(gate_grads, (0, 3, 1, 2)),
        norm_gain,
        router_weight[0],
        gate_weight[0],
        up_weight[0],
        down_weight[0],
    )
    arrived, routing, input_grad, router_grad, balance = pl.pallas_call(
        leave,
        out_shape=tuple(jax.ShapeDtypeStruct(a.shape, a.dtype) for a in outs),
        in_specs=[anywhere] * 5,
        out_specs=(hbm,) * 5,
        scratch_shapes=[pltpu.VMEM(a.shape, a.dtype) for a in outs] + [sem((2, 5))],
    )(*outs)
    return (
        arrived[None, None],
        jnp.transpose(routing, (0, 2, 3, 1)),
        input_grad[None, None],
        router_grad[None],
        balance,
    )


def solution(mesh):
    split = Mesh(
        mesh.devices.reshape(mesh.shape["section"], NZ, 2, mesh.shape["dp"]),
        ("section", "ctx_0", "ctx_1", "dp"),
    )
    tokens = P("section", "dp", CTX, None)
    return jax.shard_map(
        shards,
        mesh=split,
        in_specs=(tokens,) * 6
        + (
            P("section", None),
            P("section", None, None),
            P("section", CTX, None),
            P("section", CTX, None),
            P("section", None, CTX),
        ),
        out_specs=(tokens,) * 3 + (P("section", None, None), P("section", "dp", None)),
        check_vma=False,
    )
```

```python
import jax
import jax.numpy as jnp
from jax import lax
from jax.experimental import pallas as pl
from jax.experimental.pallas import tpu as pltpu
from jax.sharding import Mesh
from jax.sharding import PartitionSpec as P

CTX = ("ctx_0", "ctx_1")
MESH = pl.DeviceIdType.MESH
EPSILON = 1e-06
ROUTE_SCALE = 2.5
HIGH = lax.Precision.HIGHEST
F32 = jnp.float32
BF16 = jnp.bfloat16

NZ, NY, NX = 8, 8, 4
G, D = 0, 1
Z_ORDER = (
    [(G, 1, m) for m in range(4)]
    + [(G, 2, m) for m in range(4)]
    + [(D, 1, m) for m in range(2)]
    + [(G, 3, m) for m in range(4)]
    + [(D, 2, m) for m in range(2)]
    + [(G, 4, m) for m in range(2)]
    + [(D, 3, m) for m in range(2)]
    + [(D, 4, 0)]
)
Y_ORDER = [(G, 0, 0), (G, 0, 1), (D, 0, 0)]
for _q in ((G, 1), (G, 2), (G, 3), (G, 4), (D, 1), (D, 2), (G, 5), (G, 6), (D, 3), (D, 4)):
    Y_ORDER += [(_q[0], _q[1], m) for m in range(2 - _q[0])]
NZP, NYP = len(Z_ORDER), len(Y_ORDER)
E_ORDER = [(G, 4, 0), (G, 4, 0), (D, 3, 0), (D, 3, 1), (D, 4, 0)]
NE = len(E_ORDER)
G5, D3, D4 = Y_ORDER.index((G, 5, 0)), Y_ORDER.index((D, 3, 0)), Y_ORDER.index((D, 4, 0))
E_LAG = 2
Y_START = 3


def lag(hops):
    return 1 + 5 * hops // 2


def lookup(values, i):
    out = jnp.int32(values[0])
    for p in range(1, len(values)):
        if values[p] != values[p - 1]:
            out = jnp.where(i >= p, jnp.int32(values[p]), out)
    return out


def code(kind, k, m):
    return kind * 64 + k * 4 + m


def z_next_place(entry):
    kind, k, m = entry
    return Z_ORDER.index((kind, k + 1, m)) if (kind, k + 1, m) in Z_ORDER else -1

NT = (((1,), (1,)), ((), ()))
TN = (((0,), (0,)), ((), ()))
NN = (((1,), (0,)), ((), ()))


def dot(a, b, dims=NN, precision=None):
    return lax.dot_general(a, b, dims, precision=precision, preferred_element_type=F32)


def exact_dot(a, b, dims):
    rows = a.shape[0]
    one = a.astype(BF16)
    left = a - one.astype(F32)
    two = left.astype(BF16)
    three = (left - two.astype(F32)).astype(BF16)
    parts = dot(jnp.concatenate([one, two, three], axis=0), b, dims)
    return parts[2 * rows :] + parts[rows : 2 * rows] + parts[:rows]


def sigmoid(v):
    return jax.nn.sigmoid(v)


def kernel(
    first_hbm, second_hbm, upstream, picks_a, picks_b, grads, gain, router_hbm, gate, up, down,
    arrived, routing, input_grad, router_grad, balance,
    first, second, router_w, grad_out, routing_out, balance_out, wgu, wd, returned, normed, inverse, gacc, uacc, hgrad, hid, gg, ug, out, qbuf,
    cnt_src, cnt_sum, cnt, aff, csum, spread, logit,
    rp, r0, b0, b1, r1, b2, r2, r3,
    local_sem, zsend, zrecv, ysend, yrecv, dzsend, dzrecv, dysend, dyrecv,
    xsem, osend, orecv, csend, crecv, rsend, rrecv,
):
    d_model = gate.shape[0] * 2 * NZ
    hidden = gate.shape[1]
    tokens = first_hbm.shape[0]
    rows_s = gate.shape[0]
    pg, pd = rows_s // 4, hidden // 2
    block = 2 * rows_s
    length = tokens * 2 * NZ

    x = lax.axis_index("section")
    z = lax.axis_index("ctx_0")
    h = lax.axis_index("ctx_1")
    dp = lax.axis_index("dp")
    j = dp // 2
    c = dp % 2
    y = h * 4 + j
    sgn = 1 - 2 * c

    def dev(xx, zz, yy, cc):
        return (xx, zz, yy // 4, (yy % 4) * 2 + cc)

    partner = dev(x, z, y, 1 - c)
    z_next = dev(x, (z + sgn + NZ) % NZ, y, c)
    y_prev = dev(x, z, (y - sgn + NY) % NY, c)
    y_next = dev(x, z, (y + sgn + NY) % NY, c)
    x_next = dev((x + 1) % NX, z, y, c)
    x_prev = dev((x + NX - 1) % NX, z, y, c)

    def z_peer(r):
        return dev(x, (z + r) % NZ, y, c)

    def y_peer(r):
        return dev(x, z, (y + r) % NY, c)

    def count_z(r):
        return remote(cnt_src, cnt.at[r], csend.at[r], crecv.at[r], z_peer(r))

    def count_y():
        return remote(cnt_sum, cnt.at[0], csend.at[0], crecv.at[0], y_peer(NY // 2))

    def remote(src, dst, send, recv, device):
        return pltpu.make_async_remote_copy(
            src_ref=src, dst_ref=dst, send_sem=send, recv_sem=recv, device_id=device, device_id_type=MESH
        )

    barrier = pltpu.get_barrier_semaphore()

    def greet(device):
        pl.semaphore_signal(barrier, inc=1, device_id=device, device_id_type=MESH)

    greet(partner)
    greet(x_next)
    greet(x_prev)
    for r in range(1, NZ):
        greet(z_peer(r))
    for r in range(1, NY):
        greet(y_peer(r))

    own = z * 2 + h
    own_rows = pl.ds(pl.multiple_of(own * rows_s, rows_s), rows_s)
    local = [
        pltpu.make_async_copy(first_hbm, first, local_sem.at[0]),
        pltpu.make_async_copy(second_hbm, second, local_sem.at[1]),
        pltpu.make_async_copy(router_hbm, router_w, local_sem.at[2]),
        pltpu.make_async_copy(gate, wgu.at[0, own_rows, :], local_sem.at[3]),
        pltpu.make_async_copy(up, wgu.at[1, own_rows, :], local_sem.at[4]),
        pltpu.make_async_copy(down, wd.at[:, own_rows], local_sem.at[5]),
    ]
    for copy in local[3:] + local[:3]:
        copy.start()

    def g_piece(slot, p):
        start = pl.multiple_of(slot * rows_s + p * pg, pg)
        return wgu.at[:, pl.ds(start, pg), :]

    def d_piece(slot, p):
        return wd.at[pl.ds(pl.multiple_of(p * pd, pd), pd), pl.ds(pl.multiple_of(slot * rows_s, rows_s), rows_s)]

    def slot_of(zz, hh):
        return ((zz + 2 * NZ) % NZ) * 2 + hh

    def z_ref(kind, k, m, core, sign):
        slot = slot_of(z - sign * k, h)
        if kind == G:
            return g_piece(slot, (2 * core + m) % 4)
        return d_piece(slot, (core + m) % 2)

    def y_ref(kind, q, m, core, sign, hh):
        slot = slot_of(z + (1 - 2 * (q % 2)) * ((q + 1) // 2) * sign, hh)
        if kind == G:
            return g_piece(slot, 2 * core + m)
        return d_piece(slot, core)

    def e_ref(i, core, sign):
        kind, k, flip = E_ORDER[i]
        slot = slot_of(z - sign * k, 1 - h)
        if kind == G:
            return g_piece(slot, 2 * core + i)
        return d_piece(slot, (core + flip) % 2)

    def z_copy(ref, place):
        return remote(ref, ref, zsend.at[place], zrecv.at[place], z_next)

    def y_copy(ref, place):
        return remote(ref, ref, ysend.at[place], yrecv.at[place], y_next)

    def dz_copy(ref, place):
        return remote(ref, ref, dzsend.at[place], dzrecv.at[place], partner)

    def dy_copy(ref, place):
        return remote(ref, ref, dysend.at[place], dyrecv.at[place], partner)

    last = 3 * (1 - c)
    is_last = j == last
    hops = jnp.where(c == 0, j + 1, 4 - j)
    hops_max = jnp.maximum(hops, 5 - hops)
    send_half = jnp.where(is_last, h, 1 - h)

    for copy in local[3:]:
        copy.wait()
    with jax.named_scope("s_barrier"):
        pl.semaphore_wait(barrier, 3 + NZ - 1 + NY - 1)
    for m in range(3):
        z_copy(z_ref(G, 0, m, c, sgn), m).start()

    @pl.when(is_last)
    def _():
        for place in range(Y_START):
            y_copy(y_ref(*Y_ORDER[place], c, sgn, send_half), place).start()

    back = remote(upstream, returned, xsem.at[0], xsem.at[1], x_prev)
    back.start()

    step_rows = 16

    def norm_rows(source, base):
        def body(i, _):
            rows = pl.ds(pl.multiple_of(i * step_rows, step_rows), step_rows)
            values = source[rows, :].astype(F32)
            inv = lax.rsqrt(jnp.mean(values * values, axis=-1, keepdims=True) + EPSILON)
            inverse[pl.ds(pl.multiple_of(base + i * step_rows, step_rows), step_rows), :] = jnp.broadcast_to(inv, (step_rows, 128))
            scaled = (values * inv * gain[...]).astype(BF16)
            for b in range(d_model // block):
                normed[b, pl.ds(pl.multiple_of(base + i * step_rows, step_rows), step_rows), :] = scaled[:, b * block : (b + 1) * block]
            return 0

        lax.fori_loop(0, tokens // step_rows, body, 0)

    with jax.named_scope("s_norm"):
        local[0].wait()
        norm_rows(first, 0)
        local[1].wait()
        norm_rows(second, tokens)
    gacc[...] = jnp.zeros_like(gacc)
    uacc[...] = jnp.zeros_like(uacc)
    hgrad[...] = jnp.zeros_like(hgrad)

    experts = router_w.shape[0]
    top = picks_a.shape[1]
    local[2].wait()
    logits = jnp.zeros((experts, 2 * tokens), F32)
    for b in range(d_model // block):
        logits = logits + exact_dot(router_w[:, b * block : (b + 1) * block], normed[b], NT)
    affinity = sigmoid(logits)
    aff[...] = affinity
    labels = lax.broadcasted_iota(jnp.int32, (experts, tokens), 0)

    def picked(picks, affinities, k):
        hit = picks[0, k] == labels
        return jnp.sum(jnp.where(hit, affinities, 0.0), axis=0, keepdims=True), hit

    stats = []
    for m, picks in enumerate((picks_a, picks_b)):
        part = affinity[:, m * tokens : (m + 1) * tokens]
        tab = jnp.zeros((experts, tokens), F32)
        chosen = []
        for k in range(top):
            value, hit = picked(picks, part, k)
            chosen.append(value)
            tab = tab + jnp.where(hit, 1.0, 0.0)
        total = chosen[0]
        for value in chosen[1:]:
            total = total + value
        all_aff = jnp.sum(part, axis=0, keepdims=True)
        if m == 0:
            for k in range(top):
                routing_out[0, k] = ROUTE_SCALE * chosen[k] / total
        else:
            csum[...] = total
            spread[...] = all_aff
        stats.append((tab, part / all_aff))
    ones = jnp.ones((8, tokens), F32)
    counts_row = dot(ones, jnp.concatenate([stats[0][0], stats[1][0]], axis=0), NT, HIGH)
    shares_row = dot(ones, jnp.concatenate([stats[0][1], stats[1][1]], axis=0), NT, HIGH)
    row_id = lax.broadcasted_iota(jnp.int32, (8, 2 * experts), 0)
    packed = jnp.where(row_id == 0, counts_row, jnp.where(row_id == 1, shares_row, 0.0))
    cnt_src[...] = packed
    for r in range(1, NZ):
        count_z(r).start()
    z_copy(z_ref(G, 0, 3, c, sgn), 3).start()

    half_e = experts // 2
    own_half = pl.ds(pl.multiple_of(c * half_e, half_e), half_e)
    other_half = pl.ds(pl.multiple_of((1 - c) * half_e, half_e), half_e)

    def cols(i, width):
        return pl.ds(pl.multiple_of(i * width, width), width)

    def rs_pair():
        return remote(rp.at[other_half, :], b0, rsend.at[0], rrecv.at[0], partner)

    def part(i):
        return r0.at[:, cols((y + sgn * (i + 1) + 2 * NY) % NY, block)]

    def ring(i, source):
        return remote(source, b1.at[i], rsend.at[1 + i], rrecv.at[1 + i], y_prev)

    def tile(yy):
        return (cols(yy // 2, 8), cols(yy % 2, 128))

    def rs_small(r):
        return remote(r1.at[tile((z + r) % NZ)], b2.at[r], rsend.at[8 + r], rrecv.at[8 + r], z_peer(r))

    def ag_small(r):
        return remote(r2, r3.at[tile(z)], rsend.at[16 + r], rrecv.at[16 + r], z_peer(r))

    def ag_big(r):
        return remote(
            r3, router_grad.at[own_half, cols(y, block)], rsend.at[24 + r], rrecv.at[24 + r], y_peer(r)
        )

    def ag_pair():
        return remote(
            router_grad.at[own_half, :], router_grad.at[own_half, :], rsend.at[32], rrecv.at[32], partner
        )

    def router_counts():
        for r in range(1, NZ):
            count_z(r).wait_recv()
        totals = cnt_src[...]
        for r in range(1, NZ):
            totals = totals + cnt[r]
        cnt_sum[...] = totals
        count_y().start()

    def router_0():
        count_y().wait_recv()
        totals = cnt_sum[...] + cnt[0]
        scale = experts / (top * length)
        frac = scale * totals[0:1, :]
        terms = frac * totals[1:2, :] / length
        lane = lax.broadcasted_iota(jnp.int32, (1, 2 * experts), 1)
        bal_a = jnp.sum(jnp.where(lane < experts, terms, 0.0), axis=1, keepdims=True)
        bal_b = jnp.sum(jnp.where(lane >= experts, terms, 0.0), axis=1, keepdims=True)
        balance_out[0] = jnp.where(lane == 0, bal_a, bal_b)[:, 0:2]
        e_sub = lax.broadcasted_iota(jnp.int32, (experts, 2 * experts), 0)
        e_lane = lax.broadcasted_iota(jnp.int32, (experts, 2 * experts), 1)
        frac_col = jnp.sum(jnp.where(e_lane == e_sub + experts, frac, 0.0), axis=1, keepdims=True)
        aff_b = aff[:, tokens : 2 * tokens]
        chosen_sum = csum[...]
        shares = aff_b / spread[...]
        inner = jnp.zeros((1, tokens), F32)
        for k in range(top):
            value, _ = picked(picks_b, aff_b, k)
            inner = inner + grads[0, k] * value
        agrad = jnp.zeros((experts, tokens), F32)
        for k in range(top):
            hit = picks_b[0, k] == labels
            cgrad = ROUTE_SCALE * (grads[0, k] / chosen_sum - inner / (chosen_sum * chosen_sum))
            agrad = agrad + jnp.where(hit, cgrad, 0.0)
        share_grad = frac_col / length
        agrad = agrad + (share_grad - jnp.sum(share_grad * shares, axis=0, keepdims=True)) / spread[...]
        lg = agrad * aff_b * (1.0 - aff_b)
        logit[...] = lg
        for b in range(d_model // block):
            rp[:, b * block : (b + 1) * block] = exact_dot(lg, normed[b, tokens : 2 * tokens, :], NN)
        rs_pair().start()

    def router_term():
        lg_t = jnp.transpose(logit[...])
        for b in range(d_model // block):
            at = slice(b * block, (b + 1) * block)
            qbuf[b] = dot(lg_t, router_w[:, at], NN, HIGH)

    def router_1():
        rs_pair().wait_recv()
        r0[...] = rp[own_half, :] + b0[...]
        ring(0, part(0)).start()

    def ring_step(i):
        ring(i - 1, b1.at[i - 1]).wait_recv()
        b1[i - 1] = b1[i - 1] + part(i)[...]

        @pl.when(i < NZ - 1)
        def _():
            ring(i, b1.at[i - 1]).start()

        @pl.when(i == NZ - 1)
        def _():
            r1[...] = b1[i - 1]
            for r in range(1, NY):
                rs_small(r).start()

    def router_3():
        for r in range(1, NY):
            rs_small(r).wait_recv()
        acc = r1[tile(z)]
        for r in range(1, NY):
            acc = acc + b2[r]
        r2[...] = acc
        r3[tile(z)] = acc
        for r in range(1, NY):
            ag_small(r).start()

    def router_4():
        for r in range(1, NY):
            ag_small(r).wait_recv()
        pltpu.make_async_copy(r3, router_grad.at[own_half, cols(y, block)], local_sem.at[1]).start()

    def router_5():
        for r in range(1, NZ):
            ag_big(r).wait_recv()
        pltpu.make_async_copy(r3, router_grad.at[own_half, cols(y, block)], local_sem.at[1]).wait()
        ag_pair().start()

    router_at = {3: router_counts, 5: router_0, 6: router_1, 8: router_term, 22: router_3, 26: router_4}
    ring_at, ring_every, spread_at = 6, 2, 27

    n_tile = 256

    def z_rows(zz):
        return pl.ds(pl.multiple_of(zz * block, block), block)

    def g_block(zz):
        lhs = normed[zz]
        for n in range(hidden // n_tile):
            at = slice(n * n_tile, (n + 1) * n_tile)
            gacc[:, at] += dot(lhs, wgu[0, z_rows(zz), at])
            uacc[:, at] += dot(lhs, wgu[1, z_rows(zz), at])

    def make_hidden():
        def body(i, _):
            rows = cols(i, 16)
            v = gacc[rows, :]
            hid[rows, :] = (v * sigmoid(v) * uacc[rows, :]).astype(BF16)
            return 0

        lax.fori_loop(0, tokens // 16, body, 0)

    def out_send(zz):
        return remote(
            out.at[:, z_rows(zz)], arrived.at[:, z_rows(zz)], osend.at[zz], orecv.at[zz], x_next
        )

    def out_block(zz):
        acc = dot(hid[...], wd[:, z_rows(zz)])
        out[:, z_rows(zz)] = (first[:, z_rows(zz)].astype(F32) + acc).astype(BF16)
        out_send(zz).start()

    def hgrad_block(zz):
        lhs = returned[:, z_rows(zz)]
        for n in range(hidden // n_tile):
            at = slice(n * n_tile, (n + 1) * n_tile)
            hgrad[:, at] += dot(lhs, wd[at, z_rows(zz)], NT)

    def pair(fn, group):
        fn((z + group) % NZ)
        fn((z - group + NZ) % NZ)

    def on_g(q):
        @pl.when(q == 0)
        def _():
            g_block(z)

        @pl.when((q % 2 == 0) & (q > 0))
        def _():
            pair(g_block, q // 2)

    def all_g():
        g_block((z + 4) % NZ)
        make_hidden()

        def body(i, _):
            out_block((z + i + NZ - 1) % NZ)
            return 0

        lax.fori_loop(0, 3, body, 0)

    def on_d(q):
        @pl.when(q == 0)
        def _():
            back.wait_recv()
            hgrad_block(z)

        @pl.when((q % 2 == 0) & (q > 0))
        def _():
            pair(hgrad_block, q // 2)

        @pl.when(q == 4)
        def _():
            pair(out_block, 2)

    def all_d():
        pair(hgrad_block, 3)
        hgrad_block((z + 4) % NZ)
        pair(out_block, 3)
        out_block((z + 4) % NZ)

    z_codes = [code(*entry) for entry in Z_ORDER]
    y_codes = [code(*entry) for entry in Y_ORDER]
    z_follow = [z_next_place(entry) for entry in Z_ORDER]
    d1 = Z_ORDER.index((D, 1, 0))
    g2_end = 3

    def by_kind(entry, fn):
        for kind in (G, D):

            @pl.when(entry // 64 == kind)
            def _():
                fn(kind, (entry % 64) // 4, entry % 4)

    def slot(t, _):
        nz = t - 1

        @pl.when((nz >= 0) & (nz < NZP))
        def _():
            follow = lookup(z_follow, nz)

            def arrived_z(kind, k, m):
                ref = z_ref(kind, k, m, c, sgn)
                with jax.named_scope("w_z"):
                    z_copy(ref, nz).wait_recv()

                @pl.when(follow >= 0)
                def _():
                    z_copy(ref, follow).start()

                dz_copy(ref, nz).start()

            by_kind(lookup(z_codes, nz), arrived_z)

            @pl.when(nz == g2_end)
            def _():
                for m in range(2):
                    z_copy(z_ref(D, 0, m, c, sgn), d1 + m).start()

        ndz = t - 2

        @pl.when((ndz >= 0) & (ndz < NZP))
        def _():
            def arrived_dz(kind, k, m):
                with jax.named_scope("w_dz"):
                    dz_copy(z_ref(kind, k, m, 1 - c, -sgn), ndz).wait_recv()

            by_kind(lookup(z_codes, ndz), arrived_dz)

        nyr = t - lag(hops)

        @pl.when((nyr >= 0) & (nyr < NYP))
        def _():
            def arrived_y(kind, q, m):
                ref = y_ref(kind, q, m, c, sgn, 1 - h)
                with jax.named_scope("w_y"):
                    y_copy(ref, nyr).wait_recv()

                @pl.when(jnp.logical_not(is_last))
                def _():
                    y_copy(ref, nyr).start()

                dy_copy(ref, nyr).start()
                if kind == G:

                    @pl.when(q == 5)
                    def _():
                        z_copy(ref, NZP + m).start()

                else:

                    @pl.when(q == 3)
                    def _():
                        z_copy(ref, NZP + 2).start()

            by_kind(lookup(y_codes, nyr), arrived_y)

        def arrived_e(i):
            ref = e_ref(i, c, sgn)
            with jax.named_scope("w_e"):
                z_copy(ref, NZP + i).wait_recv()
            if i == 2:
                z_copy(ref, NZP + 4).start()
            dz_copy(ref, NZP + i).start()

        def arrived_de(i):
            with jax.named_scope("w_de"):
                dz_copy(e_ref(i, 1 - c, -sgn), NZP + i).wait_recv()

        late = t - lag(hops_max)
        for i, place in ((0, G5), (1, G5 + 1), (2, D3), (4, D3 + E_LAG)):

            @pl.when(late == place + E_LAG)
            def _():
                arrived_e(i)

        nys = t + 1

        @pl.when(is_last & (nys >= Y_START) & (nys < NYP))
        def _():
            def inject(kind, q, m):
                y_copy(y_ref(kind, q, m, c, sgn, h), nys).start()

            by_kind(lookup(y_codes, nys), inject)

        nyd = t - lag(hops_max) - 1

        @pl.when((nyd >= 0) & (nyd < NYP))
        def _():
            def arrived_dy(kind, q, m):
                with jax.named_scope("w_dy"):
                    dy_copy(y_ref(kind, q, m, 1 - c, -sgn, 1 - h), nyd).wait_recv()
                if kind == G:

                    @pl.when(m == 1)
                    def _():
                        with jax.named_scope("c_g"):
                            on_g(q)

                else:
                    @pl.when(q == 4)
                    def _():
                        z_copy(y_ref(kind, q, m, 1 - c, -sgn, 1 - h), NZP + 3).start()

                    with jax.named_scope("c_d"):
                        on_d(q)

            by_kind(lookup(y_codes, nyd), arrived_dy)

        @pl.when(nyd == G5 + E_LAG)
        def _():
            arrived_de(0)

        @pl.when(nyd == G5 + 1 + E_LAG)
        def _():
            arrived_de(1)
            with jax.named_scope("c_allg"):
                all_g()

        @pl.when(nyd == D3 + E_LAG)
        def _():
            arrived_de(2)

        @pl.when(nyd == D4 + E_LAG)
        def _():
            arrived_e(3)

        @pl.when(nyd == D4 + E_LAG + 1)
        def _():
            arrived_de(3)
            arrived_de(4)
            with jax.named_scope("c_alld"):
                all_d()

        ring_i = (t - ring_at) // ring_every

        @pl.when((t > ring_at) & ((t - ring_at) % ring_every == 0) & (ring_i < NZ))
        def _():
            with jax.named_scope("ring_step"):
                ring_step(ring_i)

        for at, stage in router_at.items():

            @pl.when(t == at)
            def _():
                with jax.named_scope(stage.__name__):
                    stage()

        spread_i = t - spread_at

        @pl.when((spread_i >= 0) & (spread_i < 4))
        def _():
            ag_big(4 + spread_i).start()

            @pl.when(spread_i < 3)
            def _():
                ag_big(3 - spread_i).start()

        return 0

    lax.fori_loop(0, D4 + E_LAG + 2 + lag(4) + 1, slot, 0)

    def shared_back(i, _):
        rows = cols(i, 16)
        b_rows = pl.ds(pl.multiple_of(tokens + i * 16, 16), 16)
        v, u, hg = gacc[b_rows, :], uacc[b_rows, :], hgrad[rows, :]
        s = sigmoid(v)
        gg[rows, :] = (hg * u * (s * (1.0 + v * (1.0 - s)))).astype(BF16)
        ug[rows, :] = (hg * v * s).astype(BF16)
        return 0

    with jax.named_scope("t_back"):
        lax.fori_loop(0, tokens // 16, shared_back, 0)
    def grad_block(b, mean):
        at = z_rows(b)
        grad = dot(gg[...], wgu[0, at, :], NT) + dot(ug[...], wgu[1, at, :], NT)
        q = (grad + qbuf[b]) * gain[:, at]
        qbuf[b] = q
        return mean + jnp.sum(q * second[:, at].astype(F32), axis=-1, keepdims=True)

    with jax.named_scope("router_5"):
        router_5()
    with jax.named_scope("t_grad"):
        mean = lax.fori_loop(0, d_model // block, grad_block, jnp.zeros((tokens, 1), F32), unroll=True) / d_model
    inv_b = inverse[tokens : 2 * tokens, 0:1]
    factor = inv_b * inv_b * mean

    def final_block(b, _):
        at = z_rows(b)
        values = second[:, at].astype(F32)
        part = inv_b * (qbuf[b] - values * factor)
        grad_out[:, at] = (returned[:, at].astype(F32) + part).astype(BF16)
        return 0

    with jax.named_scope("t_final"):
        lax.fori_loop(0, d_model // block, final_block, 0)

    with jax.named_scope("t_agpair"):
        ag_pair().wait_recv()
    results = [
        pltpu.make_async_copy(grad_out, input_grad, local_sem.at[0]),
        pltpu.make_async_copy(routing_out, routing, local_sem.at[2]),
        pltpu.make_async_copy(balance_out, balance, local_sem.at[3]),
    ]
    for result in results:
        result.start()

    def drain(count, body):
        def step(n, _):
            body(n)
            return 0

        lax.fori_loop(0, count, step, 0)

    with jax.named_scope("t_out"):
        drain(2 * NZ // 2, lambda n: out_send(n).wait())
    for order, copies in ((Z_ORDER + E_ORDER, (z_copy, dz_copy)), (Y_ORDER, (y_copy, dy_copy))):
        for place, entry in enumerate(order):
            ref = g_piece(0, 0) if entry[0] == G else d_piece(0, 0)
            for copy in copies:
                copy(ref, place).wait_send()
    back.wait_send()
    count_y().wait_send()
    for r in range(1, NZ):
        count_z(r).wait_send()
    rs_pair().wait_send()
    ag_pair().wait_send()
    for r in range(1, NZ):
        ring(r - 1, b1.at[0]).wait_send()
        ag_big(r).wait_send()
    for r in range(1, NY):
        rs_small(r).wait_send()
        ag_small(r).wait_send()
    for result in results:
        result.wait()


def leave(*refs):
    n = (len(refs) - 1) // 3
    sems = refs[-1]
    into = [pltpu.make_async_copy(refs[i], refs[2 * n + i], sems.at[0, i]) for i in range(n)]
    away = [pltpu.make_async_copy(refs[2 * n + i], refs[n + i], sems.at[1, i]) for i in range(n)]
    for copy in into:
        copy.start()
    for i in range(n):
        into[i].wait()
        away[i].start()
    for copy in away:
        copy.wait()


def shards(
    first_input, second_input, upstream, first_picks, second_picks, gate_grads,
    norm_gain, router_weight, gate_weight, up_weight, down_weight,
):
    tokens, d_model = first_input.shape[2:]
    hidden = gate_weight.shape[2]
    experts = router_weight.shape[1]
    top = first_picks.shape[3]
    block = d_model // NZ
    blocks = d_model // block
    vmem = pl.BlockSpec(memory_space=pltpu.VMEM)
    hbm = pl.BlockSpec(memory_space=pltpu.HBM)
    anywhere = pl.BlockSpec(memory_space=pl.ANY)
    sem = pltpu.SemaphoreType.DMA
    half = experts // 2
    outs = pl.pallas_call(
        kernel,
        out_shape=(
            jax.ShapeDtypeStruct((tokens, d_model), BF16),
            jax.ShapeDtypeStruct((1, top, 1, tokens), F32),
            jax.ShapeDtypeStruct((tokens, d_model), BF16),
            jax.ShapeDtypeStruct((experts, d_model), F32),
            jax.ShapeDtypeStruct((1, 1, 2), F32),
        ),
        in_specs=[hbm, hbm, hbm, vmem, vmem, vmem, vmem, hbm, hbm, hbm, hbm],
        out_specs=(anywhere,) * 5,
        scratch_shapes=[
            pltpu.VMEM((tokens, d_model), BF16),
            pltpu.VMEM((tokens, d_model), BF16),
            pltpu.VMEM((experts, d_model), F32),
            pltpu.VMEM((tokens, d_model), BF16),
            pltpu.VMEM((1, top, 1, tokens), F32),
            pltpu.VMEM((1, 1, 2), F32),
            pltpu.VMEM((2, d_model, hidden), BF16),
            pltpu.VMEM((hidden, d_model), BF16),
            pltpu.VMEM((tokens, d_model), BF16),
            pltpu.VMEM((blocks, 2 * tokens, block), BF16),
            pltpu.VMEM((2 * tokens, 128), F32),
            pltpu.VMEM((2 * tokens, hidden), F32),
            pltpu.VMEM((2 * tokens, hidden), F32),
            pltpu.VMEM((tokens, hidden), F32),
            pltpu.VMEM((tokens, hidden), BF16),
            pltpu.VMEM((tokens, hidden), BF16),
            pltpu.VMEM((tokens, hidden), BF16),
            pltpu.VMEM((tokens, d_model), BF16),
            pltpu.VMEM((blocks, tokens, block), F32),
            pltpu.VMEM((8, 2 * experts), F32),
            pltpu.VMEM((8, 2 * experts), F32),
            pltpu.VMEM((NZ, 8, 2 * experts), F32),
            pltpu.VMEM((experts, 2 * tokens), F32),
            pltpu.VMEM((1, tokens), F32),
            pltpu.VMEM((1, tokens), F32),
            pltpu.VMEM((experts, tokens), F32),
            pltpu.VMEM((experts, d_model), F32),
            pltpu.VMEM((half, d_model), F32),
            pltpu.VMEM((half, d_model), F32),
            pltpu.VMEM((NZ, half, block), F32),
            pltpu.VMEM((half, block), F32),
            pltpu.VMEM((NY, 8, 128), F32),
            pltpu.VMEM((8, 128), F32),
            pltpu.VMEM((half, block), F32),
            sem((6,)),
            sem((NZP + NE,)), sem((NZP + NE,)), sem((NYP,)), sem((NYP,)),
            sem((NZP + NE,)), sem((NZP + NE,)), sem((NYP,)), sem((NYP,)),
            sem((2,)), sem((NZ,)), sem((NZ,)),
            sem((NZ,)), sem((NZ,)), sem((33,)), sem((33,)),
        ],
        compiler_params=pltpu.CompilerParams(
            collective_id=0, has_side_effects=True, vmem_limit_bytes=62 * 1024 * 1024
        ),
    )(
        first_input[0, 0],
        second_input[0, 0],
        upstream[0, 0],
        jnp.transpose(first_picks, (0, 3, 1, 2)),
        jnp.transpose(second_picks, (0, 3, 1, 2)),
        jnp.transpose(gate_grads, (0, 3, 1, 2)),
        norm_gain,
        router_weight[0],
        gate_weight[0],
        up_weight[0],
        down_weight[0],
    )
    arrived, routing, input_grad, router_grad, balance = pl.pallas_call(
        leave,
        out_shape=tuple(jax.ShapeDtypeStruct(a.shape, a.dtype) for a in outs),
        in_specs=[anywhere] * 5,
        out_specs=(hbm,) * 5,
        scratch_shapes=[pltpu.VMEM(a.shape, a.dtype) for a in outs] + [sem((2, 5))],
    )(*outs)
    return (
        arrived[None, None],
        jnp.transpose(routing, (0, 2, 3, 1)),
        input_grad[None, None],
        router_grad[None],
        balance,
    )


def solution(mesh):
    split = Mesh(
        mesh.devices.reshape(mesh.shape["section"], NZ, 2, mesh.shape["dp"]),
        ("section", "ctx_0", "ctx_1", "dp"),
    )
    tokens = P("section", "dp", CTX, None)
    return jax.shard_map(
        shards,
        mesh=split,
        in_specs=(tokens,) * 6
        + (
            P("section", None),
            P("section", None, None),
            P("section", CTX, None),
            P("section", CTX, None),
            P("section", None, CTX),
        ),
        out_specs=(tokens,) * 3 + (P("section", None, None), P("section", "dp", None)),
        check_vma=False,
    )
```
